128 devices in a mesh: seq: 32 (over z_lo, y, x), grp: 4 (over z_hi, core).
Axes of the slice: x: 4, y: 4, z: 4 (z_hi: 2, z_lo: 2; z = z_hi * 2 + z_lo), core: 2. Of those that a mesh axis runs over, the one named last changes fastest.
Arguments:
- queries: bfloat16 [4, 8192, 1536], P('grp', 'seq'), may hold values from -6 to 6
- key_rows: bfloat16 [4, 8192, 1536], P('grp', 'seq'), may hold values from -6 to 6
- value_rows: bfloat16 [4, 8192, 1536], P('grp', 'seq'), may hold values from -6 to 6
- attn_cotangent: bfloat16 [4, 8192, 1536], P('grp', 'seq'), may hold values from -6 to 6
- mixer_input: bfloat16 [4, 4096, 3072], P('grp', 'seq'), may hold values from -6 to 6
- step_raw: bfloat16 [4, 4096, 3072], P('grp', 'seq'), may hold values from -3 to 3
- state_in: bfloat16 [4, 8, 4096], P('grp', None, 'seq'), may hold values from -6 to 6
- state_out: bfloat16 [4, 8, 4096], P('grp', None, 'seq'), may hold values from -6 to 6
- mixer_cotangent: bfloat16 [4, 4096, 3072], P('grp', 'seq'), may hold values from -0.3125 to 0.3125
- decay_log: float32 [8, 3072], replicated, may hold values from -9 to 0.5
- step_bias: float32 [3072], replicated, may hold values from -4 to -1
- skip_gain: float32 [3072], replicated, may hold values from 0.5 to 1.5
Outputs:
- grad_queries: bfloat16 [4, 8192, 1536], P('grp', 'seq')
- grad_keys: bfloat16 [4, 8192, 1536], P('grp', 'seq')
- grad_values: bfloat16 [4, 8192, 1536], P('grp', 'seq')
- grad_input: bfloat16 [4, 4096, 3072], P('grp', 'seq')
- grad_step: bfloat16 [4, 4096, 3072], P('grp', 'seq')
- grad_state_in: bfloat16 [4, 8, 4096], P('grp', None, 'seq')
- grad_state_out: bfloat16 [4, 8, 4096], P('grp', None, 'seq')
- grad_decay_log: float32 [8, 3072], replicated
- grad_step_bias: float32 [3072], replicated
- grad_skip_gain: float32 [3072], replicated
The draws below stay inside these ranges and needn't reach their ends.
All inputs are finite; a program needn't handle non-finite values.
Results may differ from the reference program's by a relative error of at most 0.0097.
Values may be sent and summed in bfloat16 or wider, within the bound.
A program may use at most 128 MiB of HBM per device.

```python
import jax
import jax.numpy as jnp
from jax import lax

HEADS = 12
HEAD_DIM = 128
INNER = 3072
STATE = 8
WINDOW = 1024
A_TOK = 256
TOKENS = 8192
M_TOKENS = 4096
SEQS = 4


def base_rows(key, salt):
    normal_rows = jax.random.normal(jax.random.fold_in(key, salt), (SEQS, TOKENS, HEADS * HEAD_DIM), jnp.float32)
    return jnp.clip(normal_rows, -6.0, 6.0)


def draw_queries(key, part):
    result = base_rows(key, 11)
    return result.astype(jnp.bfloat16)


def draw_key_rows(key, part):
    result = base_rows(key, 12)
    return result.astype(jnp.bfloat16)


def level_of(key, extent, cuts, least, largest):
    def one(position, shards_of):
        draws = jax.random.uniform(jax.random.fold_in(jax.random.fold_in(key, 6), position), (shards_of,), jnp.float32, least / len(cuts), largest / len(cuts))
        return jnp.repeat(jnp.exp(draws), extent[position] // shards_of).reshape((-1,) + (1,) * (len(extent) - position - 1))

    loudness = one(*cuts[0])
    for cut in cuts[1:]:
        loudness = loudness * one(*cut)
    return loudness


def bell_draw(rng, dims, deviation, most, cuts=(), kind=jnp.bfloat16):
    values = jax.random.normal(rng, dims, jnp.float32) * deviation
    if len(cuts) > 0:
        values = level_of(rng, dims, cuts, -0.22, 0.18) * values
    return jnp.clip(values, min=-most, max=most).astype(kind)


def setup_inputs(seed: int = 0) -> dict:
    key_of = jax.random.split(jax.random.key(seed), 13)
    queries = draw_queries(jax.random.fold_in(key_of[12], 71), 0)
    key_rows = draw_key_rows(jax.random.fold_in(key_of[12], 71), 0)
    value_rows = bell_draw(key_of[2], (SEQS, TOKENS, HEADS * HEAD_DIM), 1.0, 6.0, ((0, 4), (1, 32)))
    attn_cotangent = bell_draw(key_of[3], (SEQS, TOKENS, HEADS * HEAD_DIM), 1.0, 6.0, ((0, 4), (1, 32)))
    mixer_input = bell_draw(key_of[4], (SEQS, M_TOKENS, INNER), 1.0, 6.0, ((0, 4), (1, 32)))
    step_raw = bell_draw(key_of[5], (SEQS, M_TOKENS, INNER), 0.5, 3.0, ((0, 4), (1, 32)))
    state_in = bell_draw(key_of[6], (SEQS, STATE, M_TOKENS), 1.0, 6.0, ((0, 4), (2, 32)))
    state_out = bell_draw(key_of[7], (SEQS, STATE, M_TOKENS), 1.0, 6.0, ((0, 4), (2, 32)))
    mixer_cotangent = bell_draw(key_of[8], (SEQS, M_TOKENS, INNER), 0.05, 0.3125, ((0, 4), (1, 32)))
    decay_log = jnp.clip(jax.random.uniform(key_of[9], (STATE, INNER), jnp.float32, -9.0, 0.5), -9.0, 0.5)
    step_bias = jnp.clip(jax.random.uniform(key_of[10], (INNER,), jnp.float32, -4.0, -1.0), -4.0, -1.0)
    skip_gain = jnp.clip(1.0 + 0.1 * jax.random.normal(key_of[11], (INNER,), jnp.float32), 0.5, 1.5)
    return {"queries": queries, "key_rows": key_rows, "value_rows": value_rows, "attn_cotangent": attn_cotangent, "mixer_input": mixer_input, "step_raw": step_raw, "state_in": state_in, "state_out": state_out, "mixer_cotangent": mixer_cotangent, "decay_log": decay_log, "step_bias": step_bias, "skip_gain": skip_gain}


NEG_BIG = -1e+30

def window_grads(query_block, key_stack, value_stack, grad_block, first_valid):
    block_width = query_block.shape[0]
    stack_rows = key_stack.shape[0]
    lead = stack_rows - block_width
    score_scale = query_block.shape[2] ** (-0.5)
    query_wide = query_block.astype(jnp.float32)
    key_wide = key_stack.astype(jnp.float32)
    value_wide = value_stack.astype(jnp.float32)
    grad_wide = grad_block.astype(jnp.float32)
    scores = jnp.einsum('qhd,khd->hqk', query_wide, key_wide) * score_scale
    row_pos = jnp.arange(block_width)[:, None]
    col_pos = jnp.arange(stack_rows)[None, :]
    allowed = (col_pos <= row_pos + lead) & (col_pos > row_pos + lead - WINDOW) & (col_pos >= first_valid)
    scores = jnp.where(allowed[None], scores, NEG_BIG)
    row_max = lax.optimization_barrier(jnp.max(scores, axis=2, keepdims=True))
    raw_weights = jnp.exp(scores - row_max)
    softmax_prob = raw_weights / lax.optimization_barrier(jnp.sum(raw_weights, axis=2, keepdims=True))
    prob_half = lax.optimization_barrier(softmax_prob.astype(jnp.bfloat16)).astype(jnp.float32)
    output = jnp.einsum('hqk,khd->qhd', prob_half, value_wide)
    row_delta = lax.optimization_barrier(jnp.sum(output * grad_wide, axis=2))
    grad_prob = jnp.einsum('qhd,khd->hqk', grad_wide, value_wide)
    grad_score = softmax_prob * (grad_prob - row_delta.T[:, :, None])
    grad_score = lax.optimization_barrier(grad_score.astype(jnp.bfloat16)).astype(jnp.float32)
    grad_query = jnp.einsum('hqk,khd->qhd', grad_score, key_wide) * score_scale
    grad_key = jnp.einsum('hqk,qhd->khd', grad_score, query_wide) * score_scale
    grad_value = jnp.einsum('hqk,qhd->khd', prob_half, grad_wide)
    return (grad_query, grad_key, grad_value)

def attention_grads(operands):
    queries, key_rows, value_rows, grad_rows = operands
    count = TOKENS // A_TOK
    reach = (WINDOW + A_TOK - 1) // A_TOK
    shape_four = (count, A_TOK, HEADS, HEAD_DIM)
    query_blocks = queries.reshape(shape_four)
    key_blocks = key_rows.reshape(shape_four)
    value_blocks = value_rows.reshape(shape_four)
    grad_blocks = grad_rows.reshape(shape_four)
    pad_shape = (reach, A_TOK, HEADS, HEAD_DIM)
    key_padded = jnp.concatenate([jnp.zeros(pad_shape, key_blocks.dtype), key_blocks], 0)
    value_padded = jnp.concatenate([jnp.zeros(pad_shape, value_blocks.dtype), value_blocks], 0)
    stack_shape = ((reach + 1) * A_TOK, HEADS, HEAD_DIM)

    def one_block(block_index):
        query_block = lax.dynamic_index_in_dim(query_blocks, block_index, 0, keepdims=False)
        grad_block = lax.dynamic_index_in_dim(grad_blocks, block_index, 0, keepdims=False)
        key_stack = lax.dynamic_slice_in_dim(key_padded, block_index, reach + 1, 0).reshape(stack_shape)
        value_stack = lax.dynamic_slice_in_dim(value_padded, block_index, reach + 1, 0).reshape(stack_shape)
        first_valid = jnp.maximum(reach - block_index, 0) * A_TOK
        return window_grads(query_block, key_stack, value_stack, grad_block, first_valid)
    grad_query, grad_key, grad_value = lax.map(one_block, jnp.arange(count, dtype=jnp.int32))
    grad_key = grad_key.reshape(count, reach + 1, A_TOK, HEADS, HEAD_DIM)
    grad_value = grad_value.reshape(count, reach + 1, A_TOK, HEADS, HEAD_DIM)
    total_key = grad_key[:, reach]
    total_value = grad_value[:, reach]
    for distance in range(1, reach + 1):
        padding_rows = jnp.zeros((distance, A_TOK, HEADS, HEAD_DIM), jnp.float32)
        total_key = total_key + jnp.concatenate([grad_key[distance:, reach - distance], padding_rows], 0)
        total_value = total_value + jnp.concatenate([grad_value[distance:, reach - distance], padding_rows], 0)
    width = HEADS * HEAD_DIM
    return (grad_query.reshape(TOKENS, width).astype(jnp.bfloat16), total_key.reshape(TOKENS, width).astype(jnp.bfloat16), total_value.reshape(TOKENS, width).astype(jnp.bfloat16))

def mixer_forward(input_rows, raw_rows, in_proj, out_proj, decay_log, step_bias, skip_gain):
    decay_rate = -jnp.exp(decay_log)
    step_rows = jax.nn.softplus(raw_rows + step_bias)

    def advance(state, item):
        input_now, step_now, in_now, out_now = item
        state = jnp.exp(step_now[None, :] * decay_rate) * state + (step_now * input_now)[None, :] * in_now[:, None]
        return (state, lax.optimization_barrier(jnp.sum(out_now[:, None] * state, axis=0)) + skip_gain * input_now)
    zero_state = jnp.zeros(decay_log.shape, jnp.float32)
    _, output = lax.scan(advance, zero_state, (input_rows, step_rows, in_proj.T, out_proj.T))
    return output

def reference(queries, key_rows, value_rows, attn_cotangent, mixer_input, step_raw, state_in, state_out, mixer_cotangent, decay_log, step_bias, skip_gain):
    grad_queries, grad_keys, grad_values = lax.map(attention_grads, (queries, key_rows, value_rows, attn_cotangent))

    def mixer_grads(pieces):
        input_rows = pieces[0].astype(jnp.float32)
        raw_rows = pieces[1].astype(jnp.float32)
        in_proj = pieces[2].astype(jnp.float32)
        out_proj = pieces[3].astype(jnp.float32)
        cot_rows = pieces[4].astype(jnp.float32)
        _, pullback = jax.vjp(mixer_forward, input_rows, raw_rows, in_proj, out_proj, decay_log, step_bias, skip_gain)
        return pullback(cot_rows)
    grads = lax.map(mixer_grads, (mixer_input, step_raw, state_in, state_out, mixer_cotangent))
    grad_input, grad_step, grad_in, grad_out, grad_decay, grad_bias, grad_skip = grads
    return (grad_queries, grad_keys, grad_values, grad_input.astype(jnp.bfloat16), grad_step.astype(jnp.bfloat16), grad_in.astype(jnp.bfloat16), grad_out.astype(jnp.bfloat16), lax.optimization_barrier(jnp.sum(grad_decay, axis=0)), lax.optimization_barrier(jnp.sum(grad_bias, axis=0)), lax.optimization_barrier(jnp.sum(grad_skip, axis=0)))
```

```python
import functools

import jax
import jax.numpy as jnp
from jax import lax
from jax.experimental import pallas as pl
from jax.experimental.pallas import tpu as pltpu
from jax.sharding import PartitionSpec as P

MESH = pl.DeviceIdType.MESH
F32 = jnp.float32
BF16 = jnp.bfloat16

NSEQ = 32
NGRP = 4
ROW = 4
NROW = NSEQ // ROW
BLK = 256
OWN = ROW * BLK
HPD = 3
HD = 128
TOK = 128
NCH = 8
LEN = TOK // NCH
PITCH = 24
NST = 8
TILES = 24
INNER = TILES * 128
LOG2E = 1.4426950408889634
LN2 = 0.6931471805599453
NEG = -1e30
SCALE = HD**-0.5

NT = (((1,), (1,)), ((), ()))
NN = (((1,), (0,)), ((), ()))
TN = (((0,), (0,)), ((), ()))


def dot(a, b, dims):
    return lax.dot_general(a, b, dims, preferred_element_type=F32)


def kernel(
    q_hbm, k_hbm, v_hbm, do_hbm, x_ref, raw_ref, bin_ref, cout_ref, cot_ref, dl_ref, bias_ref, skip_ref,
    dq_hbm, dk_hbm, dv_hbm, gx_ref, gr_ref, gin_ref, gout_ref, gdec_ref, gbias_ref, gskip_ref,
    qs, dos, ks, vs, acc, qout, retout, retin, fin,
    dts, xs, cts, sgs, avs, a2s, btab, ctab, natt, tscr, pds, pes, sds, sbs, tot, gath, cbuf, cin,
    ahs, gxt, grt, gbacc, gcacc, gred, par, pgat, psm, p4, pfin, pout,
    in_send, in_recv, in_loc, fw_send, fw_recv, rt_send, rt_recv, q_send, q_recv, o_send, o_recv, o_loc,
    a_send, a_recv, b_send, b_recv, c_send, c_recv, d_send, d_recv, e_send, e_recv,
):
    s = lax.axis_index("seq")
    g = lax.axis_index("grp")
    col = lax.rem(s, ROW)
    base = s - col
    row = s // ROW
    first = row == 0
    last = row == NROW - 1

    barrier = pltpu.get_barrier_semaphore()

    @pl.loop(0, NSEQ)
    def _(i):
        @pl.when(i != s)
        def _():
            pl.semaphore_signal(barrier, inc=1, device_id={"seq": i}, device_id_type=MESH)

    @pl.loop(0, NGRP)
    def _(i):
        @pl.when(i != g)
        def _():
            pl.semaphore_signal(barrier, inc=1, device_id={"grp": i}, device_id_type=MESH)

    pl.semaphore_wait(barrier, NSEQ + NGRP - 2)

    srcs = (k_hbm, v_hbm, q_hbm, do_hbm)
    dsts = (ks, vs, qs, dos)
    lead = (OWN, OWN, 0, 0)

    def in_copy(t, h, off):
        peer = lax.rem(col + off, ROW)
        lanes = pl.ds(pl.multiple_of((peer * HPD + h) * HD, HD), HD)
        rows = pl.ds(pl.multiple_of(lead[t] + col * BLK, BLK), BLK)
        return pltpu.make_async_remote_copy(
            src_ref=srcs[t].at[0, :, lanes],
            dst_ref=dsts[t].at[h, rows, :],
            send_sem=in_send.at[t, h, off - 1],
            recv_sem=in_recv.at[t, h, off - 1],
            device_id={"seq": base + peer},
            device_id_type=MESH,
        )

    def in_wait(t, h, off):
        peer = lax.rem(col + ROW - off, ROW)
        lanes = pl.ds(pl.multiple_of((col * HPD + h) * HD, HD), HD)
        rows = pl.ds(pl.multiple_of(lead[t] + peer * BLK, BLK), BLK)
        pltpu.make_async_remote_copy(
            src_ref=srcs[t].at[0, :, lanes],
            dst_ref=dsts[t].at[h, rows, :],
            send_sem=in_send.at[t, h, off - 1],
            recv_sem=in_recv.at[t, h, off - 1],
            device_id={"seq": base + peer},
            device_id_type=MESH,
        ).wait_recv()

    def in_local(t, h):
        lanes = pl.ds(pl.multiple_of((col * HPD + h) * HD, HD), HD)
        rows = pl.ds(pl.multiple_of(lead[t] + col * BLK, BLK), BLK)
        return pltpu.make_async_copy(
            srcs[t].at[0, :, lanes], dsts[t].at[h, rows, :], in_loc.at[t, h]
        )

    def send_in(h):
        for t in range(4):
            for off in range(1, ROW):
                in_copy(t, h, off).start()
            in_local(t, h).start()

    def fw_copy(t, h):
        return pltpu.make_async_remote_copy(
            src_ref=dsts[t].at[h, pl.ds(OWN, OWN), :],
            dst_ref=dsts[t].at[h, pl.ds(0, OWN), :],
            send_sem=fw_send.at[t, h],
            recv_sem=fw_recv.at[t, h],
            device_id={"seq": lax.rem(s + ROW, NSEQ)},
            device_id_type=MESH,
        )

    def forward_kv(h):
        for t in range(2):
            for off in range(1, ROW):
                in_wait(t, h, off)
            in_local(t, h).wait()

            @pl.when(jnp.logical_not(last))
            def _():
                fw_copy(t, h).start()

    def rt_copy(t, h):
        return pltpu.make_async_remote_copy(
            src_ref=retout.at[h, t],
            dst_ref=retin.at[h, t],
            send_sem=rt_send.at[t, h],
            recv_sem=rt_recv.at[t, h],
            device_id={"seq": lax.rem(s + NSEQ - ROW, NSEQ)},
            device_id_type=MESH,
        )

    outs = (dk_hbm, dv_hbm)

    def out_copy(src, dst, h, off, send, recv):
        peer = lax.rem(col + off, ROW)
        lanes = pl.ds(pl.multiple_of((col * HPD + h) * HD, HD), HD)
        rows = pl.ds(pl.multiple_of(peer * BLK, BLK), BLK)
        return pltpu.make_async_remote_copy(
            src_ref=src.at[rows, :],
            dst_ref=dst.at[0, :, lanes],
            send_sem=send,
            recv_sem=recv,
            device_id={"seq": base + peer},
            device_id_type=MESH,
        )

    def out_wait(src, dst, h, off, send, recv):
        peer = lax.rem(col + ROW - off, ROW)
        lanes = pl.ds(pl.multiple_of((peer * HPD + h) * HD, HD), HD)
        pltpu.make_async_remote_copy(
            src_ref=src.at[pl.ds(0, BLK), :],
            dst_ref=dst.at[0, :, lanes],
            send_sem=send,
            recv_sem=recv,
            device_id={"seq": base + peer},
            device_id_type=MESH,
        ).wait_recv()

    def out_local(src, dst, h, sem):
        lanes = pl.ds(pl.multiple_of((col * HPD + h) * HD, HD), HD)
        rows = pl.ds(pl.multiple_of(col * BLK, BLK), BLK)
        return pltpu.make_async_copy(src.at[rows, :], dst.at[0, :, lanes], sem)

    def attention(h):
        for t in range(2, 4):
            for off in range(1, ROW):
                in_wait(t, h, off)
            in_local(t, h).wait()

        @pl.when(jnp.logical_not(first))
        def _():
            for t in range(2):
                fw_copy(t, h).wait_recv()

        @pl.when(first)
        def _():
            zeros = jnp.zeros((OWN, HD), BF16)
            ks[h, pl.ds(0, OWN), :] = zeros
            vs[h, pl.ds(0, OWN), :] = zeros

        acc[h] = jnp.zeros(acc.shape[1:], F32)
        key_pos = lax.broadcasted_iota(jnp.int32, (BLK, BLK), 0)
        qry_pos = lax.broadcasted_iota(jnp.int32, (BLK, BLK), 1)
        causal = key_pos <= qry_pos

        @pl.loop(0, ROW)
        def _(i):
            at = pl.multiple_of(i * BLK, BLK)
            qrows = pl.ds(at, BLK)
            krows = pl.ds(at, OWN + BLK)
            qb = qs[h, qrows, :]
            dob = dos[h, qrows, :]
            kb = ks[h, krows, :]
            vb = vs[h, krows, :]
            st = dot(kb, qb, NT)
            dpt = dot(vb, dob, NT)

            def bias(kt):
                return jnp.where(jnp.logical_and(first, i + kt < ROW), NEG, 0.0).astype(F32)

            parts = [jnp.where(causal, st[OWN:], st[:BLK] + bias(0))]
            for kt in range(1, ROW):
                parts.append(st[kt * BLK : (kt + 1) * BLK] + bias(kt))
            scores = jnp.concatenate(parts, 0)
            dp = jnp.concatenate([jnp.where(causal, dpt[OWN:], dpt[:BLK]), dpt[BLK:OWN]], 0)
            top = jnp.max(scores, axis=0, keepdims=True)
            raw = jnp.exp2((scores - top) * (SCALE * LOG2E))
            prob = raw * (1.0 / jnp.sum(raw, axis=0, keepdims=True))
            pb = prob.astype(BF16)
            delta = jnp.sum(pb.astype(F32) * dp, axis=0, keepdims=True)
            ds = prob * (dp - delta)
            zero = jnp.zeros((BLK, BLK), F32)
            pfull = jnp.concatenate(
                [jnp.where(causal, zero, prob[:BLK]).astype(BF16), pb[BLK:], jnp.where(causal, prob[:BLK], zero).astype(BF16)], 0
            )
            dsb = ds.astype(BF16)
            dfull = jnp.concatenate(
                [jnp.where(causal, zero, ds[:BLK]).astype(BF16), dsb[BLK:], jnp.where(causal, ds[:BLK], zero).astype(BF16)], 0
            )
            acc[h, 1, krows, :] += dot(pfull, dob, NN)
            acc[h, 0, krows, :] += dot(dfull, qb, NN)
            dq = dot(kb, dfull, TN)
            qout[h, qrows, :] = (dq.T * SCALE).astype(BF16)

        for off in range(1, ROW):
            out_copy(qout.at[h], dq_hbm, h, off, q_send.at[h, off - 1], q_recv.at[h, off - 1]).start()
        out_local(qout.at[h], dq_hbm, h, o_loc.at[2, h]).start()

        @pl.when(jnp.logical_not(first))
        def _():
            retout[h, 0] = (acc[h, 0, pl.ds(0, OWN), :] * SCALE).astype(BF16)
            rt_copy(0, h).start()
            retout[h, 1] = acc[h, 1, pl.ds(0, OWN), :].astype(BF16)
            rt_copy(1, h).start()

    def finish_head(h):
        for t in range(2):
            scale = SCALE if t == 0 else 1.0

            @pl.when(last)
            def _():
                fin[h, t] = (acc[h, t, pl.ds(OWN, OWN), :] * scale).astype(BF16)

            @pl.when(jnp.logical_not(last))
            def _():
                rt_copy(t, h).wait_recv()
                own = acc[h, t, pl.ds(OWN, OWN), :] * scale
                fin[h, t] = (own + retin[h, t].astype(F32)).astype(BF16)

            for off in range(1, ROW):
                out_copy(fin.at[h, t], outs[t], h, off, o_send.at[t, h, off - 1], o_recv.at[t, h, off - 1]).start()
            out_local(fin.at[h, t], outs[t], h, o_loc.at[t, h]).start()

    def drain():
        @pl.loop(0, HPD)
        def _(h):
            for t in range(4):
                for off in range(1, ROW):
                    in_copy(t, h, off).wait_send()
            for off in range(1, ROW):
                out_copy(qout.at[h], dq_hbm, h, off, q_send.at[h, off - 1], q_recv.at[h, off - 1]).wait_send()
                out_wait(qout.at[h], dq_hbm, h, off, q_send.at[h, off - 1], q_recv.at[h, off - 1])
            out_local(qout.at[h], dq_hbm, h, o_loc.at[2, h]).wait()
            for t in range(2):

                @pl.when(jnp.logical_not(last))
                def _():
                    fw_copy(t, h).wait_send()

                @pl.when(jnp.logical_not(first))
                def _():
                    rt_copy(t, h).wait_send()

                for off in range(1, ROW):
                    sems = (o_send.at[t, h, off - 1], o_recv.at[t, h, off - 1])
                    out_copy(fin.at[h, t], outs[t], h, off, *sems).wait_send()
                    out_wait(fin.at[h, t], outs[t], h, off, *sems)
                out_local(fin.at[h, t], outs[t], h, o_loc.at[t, h]).wait()

    def mixer_tables():
        bin32 = bin_ref[0].astype(F32)
        cout32 = cout_ref[0].astype(F32)
        for tab, rows32 in ((btab, bin32), (ctab, cout32)):
            for n in range(NST):
                wide = jnp.broadcast_to(rows32[n : n + 1, :], (TOK, TOK)).T
                for k in range(NCH):
                    natt[pl.ds(k * PITCH, LEN), :] = wide[k * LEN : (k + 1) * LEN]
                for j in range(LEN):
                    tab[n, j] = natt[pl.ds(j, NCH, stride=PITCH), :]

    def spread(block, n):
        return jnp.broadcast_to(block[n : n + 1, :], (NCH, 128))

    def mixer_local(c):
        lanes = pl.ds(pl.multiple_of(c * 128, 128), 128)
        x = x_ref[0, :, lanes].astype(F32)
        z = raw_ref[0, :, lanes].astype(F32) + bias_ref[:, lanes]
        ct = cot_ref[0, :, lanes].astype(F32)
        small = jnp.exp(-jnp.abs(z))
        dt = jnp.maximum(z, 0.0) + jnp.log1p(small)
        sg = jnp.where(z >= 0.0, 1.0, small) / (1.0 + small)
        par[c, 9:10, :] = jnp.sum(ct * x, axis=0, keepdims=True)
        for k in range(NCH):
            rows = pl.ds(k * PITCH, LEN)
            part = slice(k * LEN, (k + 1) * LEN)
            dts[c, rows, :] = dt[part]
            xs[c, rows, :] = x[part]
            cts[c, rows, :] = ct[part]
            sgs[c, rows, :] = sg[part]
        a2 = -jnp.exp(dl_ref[:, lanes]) * LOG2E
        a2s[c] = a2
        rate = [spread(a2, n) for n in range(NST)]
        state = [jnp.zeros((NCH, 128), F32) for _ in range(NST)]
        decay = [jnp.ones((NCH, 128), F32) for _ in range(NST)]
        back = [jnp.zeros((NCH, 128), F32) for _ in range(NST)]
        for j in range(LEN):
            rows = pl.ds(j, NCH, stride=PITCH)
            dtj = dts[c, rows, :]
            uj = dtj * xs[c, rows, :]
            cj = cts[c, rows, :]
            for n in range(NST):
                a = jnp.exp2(dtj * rate[n])
                avs[c, j, n] = a
                state[n] = a * state[n] + uj * btab[n, j]
                decay[n] = a * decay[n]
                back[n] = back[n] + decay[n] * (cj * ctab[n, j])
        for n in range(NST):
            rows = pl.ds(n * NCH, NCH)
            tscr[0, rows, :] = state[n]
            tscr[1, rows, :] = decay[n]
            tscr[2, rows, :] = back[n]
        ek = [tscr[0, pl.ds(k, NST, stride=NCH), :] for k in range(NCH)]
        dk = [tscr[1, pl.ds(k, NST, stride=NCH), :] for k in range(NCH)]
        bk = [tscr[2, pl.ds(k, NST, stride=NCH), :] for k in range(NCH)]
        pd = jnp.ones((NST, 128), F32)
        pe = jnp.zeros((NST, 128), F32)
        for k in range(NCH):
            pds[c, k] = pd
            pes[c, k] = pe
            pe = dk[k] * pe + ek[k]
            pd = dk[k] * pd
        sd = jnp.ones((NST, 128), F32)
        sb = jnp.zeros((NST, 128), F32)
        for k in reversed(range(NCH)):
            sds[c, k] = sd
            sbs[c, k] = sb
            sb = dk[k] * sb + bk[k]
            sd = dk[k] * sd
        tot[c, 0:8, :] = pe
        tot[c, 8:16, :] = pd
        tot[c, 16:24, :] = sb

    def scatter(src, dst, send, recv):
        @pl.loop(0, TILES)
        def _(j):
            @pl.when(j != s)
            def _():
                pltpu.make_async_remote_copy(
                    src_ref=src.at[j], dst_ref=dst.at[s], send_sem=send, recv_sem=recv,
                    device_id={"seq": j}, device_id_type=MESH,
                ).start()

        @pl.when(s < TILES)
        def _():
            dst[s] = src[s]

    def scatter_wait_recv(dst, sem):
        head = dst.at[pl.ds(0, NSEQ - 1)]
        pltpu.make_async_copy(head, head, sem).wait()

    def tiles_wait(ref, sem):
        @pl.when(s < TILES)
        def _():
            part = ref.at[pl.ds(0, TILES - 1)]
            pltpu.make_async_copy(part, part, sem).wait()

        @pl.when(s >= TILES)
        def _():
            part = ref.at[pl.ds(0, TILES)]
            pltpu.make_async_copy(part, part, sem).wait()

    def spread_out(src_of, dst, send, recv):
        @pl.loop(0, NSEQ)
        def _(i):
            @pl.when(i != s)
            def _():
                pltpu.make_async_remote_copy(
                    src_ref=src_of(i), dst_ref=dst.at[s], send_sem=send, recv_sem=recv,
                    device_id={"seq": i}, device_id_type=MESH,
                ).start()

    def mixer_prefix():
        @pl.when(s < TILES)
        def _():
            scatter_wait_recv(gath, a_recv)
            carry = jnp.zeros((NST, 128), F32)
            for i in range(NSEQ):
                cbuf[i, 0:8, :] = carry
                carry = gath[i, 8:16, :] * carry + gath[i, 0:8, :]
            carry = jnp.zeros((NST, 128), F32)
            for i in reversed(range(NSEQ)):
                cbuf[i, 8:16, :] = carry
                carry = gath[i, 8:16, :] * carry + gath[i, 16:24, :]
            spread_out(lambda i: cbuf.at[i], cin, b_send, b_recv)
            cin[s] = cbuf[s]

    def mixer_back(c):
        lanes = pl.ds(pl.multiple_of(c * 128, 128), 128)
        hin = cin[c, 0:8, :]
        gin = cin[c, 8:16, :]
        for k in range(NCH):
            rows = pl.ds(k * NST, NST)
            tscr[0, rows, :] = pds[c, k] * hin + pes[c, k]
            tscr[1, rows, :] = sds[c, k] * gin + sbs[c, k]
        state = [tscr[0, pl.ds(n, NCH, stride=NST), :] for n in range(NST)]
        a2 = a2s[c]
        for j in range(LEN):
            rows = pl.ds(j, NCH, stride=PITCH)
            uj = dts[c, rows, :] * xs[c, rows, :]
            cj = cts[c, rows, :]
            for n in range(NST):
                ah = avs[c, j, n] * state[n]
                ahs[j, n] = ah
                state[n] = ah + uj * btab[n, j]
                gcacc[n, pl.ds(j * NCH, NCH), :] += cj * state[n]
        adj = [tscr[1, pl.ds(n, NCH, stride=NST), :] for n in range(NST)]
        ga = [jnp.zeros((NCH, 128), F32) for _ in range(NST)]
        rate = [spread(a2, n) for n in range(NST)]
        skip = jnp.broadcast_to(skip_ref[:, lanes], (NCH, 128))
        gb = jnp.zeros((NCH, 128), F32)
        for j in reversed(range(LEN)):
            rows = pl.ds(j, NCH, stride=PITCH)
            dtj = dts[c, rows, :]
            xj = xs[c, rows, :]
            uj = dtj * xj
            cj = cts[c, rows, :]
            proj = None
            gdt = None
            for n in range(NST):
                gn = adj[n] + ctab[n, j] * cj
                gbacc[n, pl.ds(j * NCH, NCH), :] += gn * uj
                w = gn * ahs[j, n]
                ga[n] = ga[n] + w * dtj
                p1 = gn * btab[n, j]
                p2 = w * rate[n]
                proj = p1 if proj is None else proj + p1
                gdt = p2 if gdt is None else gdt + p2
                adj[n] = avs[c, j, n] * gn
            gxt[rows, :] = skip * cj + dtj * proj
            graw = (xj * proj + gdt * LN2) * sgs[c, rows, :]
            grt[rows, :] = graw
            gb = gb + graw
        for n in range(NST):
            tscr[2, pl.ds(n * NCH, NCH), :] = ga[n]
        gsum = tscr[2, pl.ds(0, NST, stride=NCH), :]
        for k in range(1, NCH):
            gsum = gsum + tscr[2, pl.ds(k, NST, stride=NCH), :]
        par[c, 0:8, :] = gsum * (a2 * LN2)
        par[c, 8:9, :] = jnp.sum(gb, axis=0, keepdims=True)
        for k in range(NCH):
            rows = pl.ds(k * PITCH, LEN)
            gx_ref[0, pl.ds(k * LEN, LEN), lanes] = gxt[rows, :].astype(BF16)
            gr_ref[0, pl.ds(k * LEN, LEN), lanes] = grt[rows, :].astype(BF16)

    def mixer_state_grads():
        ones = jnp.ones((8, 128), F32)
        for accum, ref in ((gbacc, gin_ref), (gcacc, gout_ref)):
            for n in range(NST):
                rows = [accum[n, pl.ds(k, LEN, stride=NCH), :] for k in range(NCH)]
                full = jnp.concatenate(rows, 0)
                line = lax.dot_general(
                    ones, full, NT, preferred_element_type=F32, precision=lax.Precision.HIGHEST
                )
                gred[n : n + 1, :] = line[0:1, :]
            ref[0] = gred[...].astype(BF16)

    def params_rows():
        @pl.when(s < TILES)
        def _():
            scatter_wait_recv(pgat, c_recv)
            total = pgat[0]
            for i in range(1, NSEQ):
                total = total + pgat[i]
            psm[...] = total
            p4[g] = total

            @pl.loop(0, NGRP)
            def _(i):
                @pl.when(i != g)
                def _():
                    pltpu.make_async_remote_copy(
                        src_ref=psm, dst_ref=p4.at[g], send_sem=d_send, recv_sem=d_recv,
                        device_id={"grp": i}, device_id_type=MESH,
                    ).start()

    def params_groups():
        @pl.when(s < TILES)
        def _():
            head = p4.at[pl.ds(0, NGRP - 1)]
            pltpu.make_async_copy(head, head, d_recv).wait()
            final = (p4[0] + p4[1]) + (p4[2] + p4[3])
            pfin[...] = final
            pout[s] = final
            spread_out(lambda i: pfin, pout, e_send, e_recv)

    def params_store():
        tiles_wait(pout, e_recv)

        @pl.loop(0, TILES)
        def _(c):
            lanes = pl.ds(pl.multiple_of(c * 128, 128), 128)
            gdec_ref[:, lanes] = pout[c, 0:8, :]
            gbias_ref[:, lanes] = pout[c, 8:9, :]
            gskip_ref[:, lanes] = pout[c, 9:10, :]

    def mixer_drain():
        tiles_wait(tot, a_send)
        tiles_wait(par, c_send)

        @pl.when(s < TILES)
        def _():
            part = cbuf.at[pl.ds(0, NSEQ - 1)]
            pltpu.make_async_copy(part, part, b_send).wait()
            part = p4.at[pl.ds(0, NGRP - 1)]
            pltpu.make_async_copy(part, part, d_send).wait()
            part = pgat.at[pl.ds(0, NSEQ - 1)]
            pltpu.make_async_copy(part, part, e_send).wait()

    send_in(0)
    mixer_tables()

    @pl.loop(0, TILES)
    def _(c):
        mixer_local(c)

    scatter(tot, gath, a_send, a_recv)
    send_in(1)
    send_in(2)
    forward_kv(0)
    mixer_prefix()
    gbacc[...] = jnp.zeros(gbacc.shape, F32)
    gcacc[...] = jnp.zeros(gcacc.shape, F32)
    par[:, 10:16, :] = jnp.zeros((TILES, 6, 128), F32)
    forward_kv(1)
    tiles_wait(cin, b_recv)

    @pl.loop(0, TILES)
    def _(c):
        mixer_back(c)

    scatter(par, pgat, c_send, c_recv)
    forward_kv(2)
    mixer_state_grads()
    params_rows()
    attention(0)
    params_groups()
    attention(1)
    finish_head(0)
    params_store()
    attention(2)
    finish_head(1)
    mixer_drain()
    finish_head(2)
    drain()


def per_device(queries, keys, values, cot_attn, x, raw, bin_, cout, cot, decay_log, step_bias, skip_gain):
    vm = pl.BlockSpec(memory_space=pltpu.VMEM)
    hbm = pl.BlockSpec(memory_space=pl.ANY)
    att = jax.ShapeDtypeStruct((1, BLK, 12 * HD), BF16)
    mix = jax.ShapeDtypeStruct((1, TOK, INNER), BF16)
    stt = jax.ShapeDtypeStruct((1, NST, TOK), BF16)
    chan = jax.ShapeDtypeStruct((1, INNER), F32)
    V = pltpu.VMEM
    D = pltpu.SemaphoreType.DMA
    scratch = [
        V((HPD, OWN, HD), BF16), V((HPD, OWN, HD), BF16), V((HPD, 2 * OWN, HD), BF16), V((HPD, 2 * OWN, HD), BF16),
        V((HPD, 2, 2 * OWN, HD), F32), V((HPD, OWN, HD), BF16),
        V((HPD, 2, OWN, HD), BF16), V((HPD, 2, OWN, HD), BF16), V((HPD, 2, OWN, HD), BF16),
        *[V((TILES, NCH * PITCH, 128), F32)] * 4,
        V((TILES, LEN, NST, NCH, 128), F32), V((TILES, NST, 128), F32),
        V((NST, LEN, NCH, 128), F32), V((NST, LEN, NCH, 128), F32), V((NCH * PITCH, 128), F32),
        V((3, NST * NCH, 128), F32),
        *[V((TILES, NCH, NST, 128), F32)] * 4,
        V((TILES, 24, 128), F32), V((NSEQ, 24, 128), F32), V((NSEQ, 16, 128), F32), V((TILES, 16, 128), F32),
        V((LEN, NST, NCH, 128), F32), V((NCH * PITCH, 128), F32), V((NCH * PITCH, 128), F32),
        V((NST, LEN * NCH, 128), F32), V((NST, LEN * NCH, 128), F32), V((NST, 128), F32),
        V((TILES, 16, 128), F32), V((NSEQ, 16, 128), F32), V((16, 128), F32), V((NGRP, 16, 128), F32),
        V((16, 128), F32), V((TILES, 16, 128), F32),
        D((4, HPD, ROW - 1)), D((4, HPD, ROW - 1)), D((4, HPD)),
        D((2, HPD)), D((2, HPD)), D((2, HPD)), D((2, HPD)),
        D((HPD, ROW - 1)), D((HPD, ROW - 1)), D((2, HPD, ROW - 1)), D((2, HPD, ROW - 1)), D((3, HPD)),
        *[D(())] * 10,
    ]
    res = pl.pallas_call(
        kernel,
        out_shape=(att, att, att, mix, mix, stt, stt, jax.ShapeDtypeStruct((NST, INNER), F32), chan, chan),
        in_specs=[hbm] * 4 + [vm] * 8,
        out_specs=(hbm,) * 3 + (vm,) * 7,
        scratch_shapes=scratch,
        compiler_params=pltpu.CompilerParams(
            collective_id=0, has_side_effects=True, vmem_limit_bytes=63 * 1024 * 1024
        ),
    )(queries, keys, values, cot_attn, x, raw, bin_, cout, cot, decay_log, step_bias.reshape(1, -1), skip_gain.reshape(1, -1))
    return tuple(res[:8]) + (res[8].reshape(-1), res[9].reshape(-1))


def solution(mesh):
    tok = P("grp", "seq", None)
    stt = P("grp", None, "seq")
    return jax.shard_map(
        per_device,
        mesh=mesh,
        in_specs=(tok,) * 4 + (tok, tok, stt, stt, tok, P(), P(), P()),
        out_specs=(tok,) * 3 + (tok, tok, stt, stt, P(), P(), P()),
        check_vma=False,
    )
```

```python
import functools

import jax
import jax.numpy as jnp
from jax import lax
from jax.experimental import pallas as pl
from jax.experimental.pallas import tpu as pltpu
from jax.sharding import PartitionSpec as P

MESH = pl.DeviceIdType.MESH
F32 = jnp.float32
BF16 = jnp.bfloat16

NSEQ = 32
NGRP = 4
ROW = 4
NROW = NSEQ // ROW
BLK = 256
OWN = ROW * BLK
HPD = 3
HD = 128
TOK = 128
NCH = 8
LEN = TOK // NCH
PITCH = 24
NST = 8
TILES = 24
INNER = TILES * 128
LOG2E = 1.4426950408889634
LN2 = 0.6931471805599453
NEG = -1e30
SCALE = HD**-0.5

NT = (((1,), (1,)), ((), ()))
NN = (((1,), (0,)), ((), ()))
TN = (((0,), (0,)), ((), ()))


def dot(a, b, dims):
    return lax.dot_general(a, b, dims, preferred_element_type=F32)


def kernel(
    q_hbm, k_hbm, v_hbm, do_hbm, x_ref, raw_ref, bin_ref, cout_ref, cot_ref, dl_ref, bias_ref, skip_ref,
    dq_hbm, dk_hbm, dv_hbm, gx_ref, gr_ref, gin_ref, gout_ref, gdec_ref, gbias_ref, gskip_ref,
    qs, dos, ks, vs, acc, qout, retout, retin, fin,
    dts, xs, cts, sgs, avs, a2s, btab, ctab, natt, tscr, pds, pes, sds, sbs, tot, gath, cbuf, cin,
    ahs, gxt, grt, gbacc, gcacc, gred, par, pgat, psm, p4, pfin, pout,
    in_send, in_recv, in_loc, fw_send, fw_recv, rt_send, rt_recv, o_send, o_recv, o_loc,
    a_send, a_recv, b_send, b_recv, c_send, c_recv, d_send, d_recv, e_send, e_recv,
):
    s = lax.axis_index("seq")
    g = lax.axis_index("grp")
    col = lax.rem(s, ROW)
    base = s - col
    row = s // ROW
    first = row == 0
    last = row == NROW - 1

    barrier = pltpu.get_barrier_semaphore()

    @pl.loop(0, NSEQ)
    def _(i):
        @pl.when(i != s)
        def _():
            pl.semaphore_signal(barrier, inc=1, device_id={"seq": i}, device_id_type=MESH)

    @pl.loop(0, NGRP)
    def _(i):
        @pl.when(i != g)
        def _():
            pl.semaphore_signal(barrier, inc=1, device_id={"grp": i}, device_id_type=MESH)

    pl.semaphore_wait(barrier, NSEQ + NGRP - 2)

    srcs = (k_hbm, v_hbm, q_hbm, do_hbm)
    dsts = (ks, vs, qs, dos)
    lead = (OWN, OWN, 0, 0)

    def in_copy(t, h, off):
        peer = lax.rem(col + off, ROW)
        lanes = pl.ds(pl.multiple_of((peer * HPD + h) * HD, HD), HD)
        rows = pl.ds(pl.multiple_of(lead[t] + col * BLK, BLK), BLK)
        return pltpu.make_async_remote_copy(
            src_ref=srcs[t].at[0, :, lanes],
            dst_ref=dsts[t].at[h, rows, :],
            send_sem=in_send.at[t, h, off - 1],
            recv_sem=in_recv.at[t, h, off - 1],
            device_id={"seq": base + peer},
            device_id_type=MESH,
        )

    def in_wait(t, h, off):
        peer = lax.rem(col + ROW - off, ROW)
        lanes = pl.ds(pl.multiple_of((col * HPD + h) * HD, HD), HD)
        rows = pl.ds(pl.multiple_of(lead[t] + peer * BLK, BLK), BLK)
        pltpu.make_async_remote_copy(
            src_ref=srcs[t].at[0, :, lanes],
            dst_ref=dsts[t].at[h, rows, :],
            send_sem=in_send.at[t, h, off - 1],
            recv_sem=in_recv.at[t, h, off - 1],
            device_id={"seq": base + peer},
            device_id_type=MESH,
        ).wait_recv()

    def in_local(t, h):
        lanes = pl.ds(pl.multiple_of((col * HPD + h) * HD, HD), HD)
        rows = pl.ds(pl.multiple_of(lead[t] + col * BLK, BLK), BLK)
        return pltpu.make_async_copy(
            srcs[t].at[0, :, lanes], dsts[t].at[h, rows, :], in_loc.at[t, h]
        )

    def send_in(t, h):
        for off in range(1, ROW):
            in_copy(t, h, off).start()
        in_local(t, h).start()

    def block_rows(start, j):
        return pl.ds(pl.multiple_of(start + j * BLK, BLK), BLK)

    def fw_copy(t, h, j, own=False):
        lanes = pl.ds(pl.multiple_of((col * HPD + h) * HD, HD), HD)
        return pltpu.make_async_remote_copy(
            src_ref=srcs[t].at[0, :, lanes] if own else dsts[t].at[h, block_rows(OWN, j), :],
            dst_ref=dsts[t].at[h, block_rows(0, j), :],
            send_sem=fw_send.at[t, h, j],
            recv_sem=fw_recv.at[t, h, j],
            device_id={"seq": lax.rem(s + ROW, NSEQ)},
            device_id_type=MESH,
        )

    def forward_own(h):
        @pl.when(jnp.logical_not(last))
        def _():
            for t in range(2):
                fw_copy(t, h, col, own=True).start()

    def forward_rest(h):
        for off in range(1, ROW):
            for t in range(2):
                in_wait(t, h, off)

            @pl.when(jnp.logical_not(last))
            def _():
                for t in range(2):
                    fw_copy(t, h, lax.rem(col + ROW - off, ROW)).start()

    def rt_copy(t, h, j):
        return pltpu.make_async_remote_copy(
            src_ref=retout.at[h, t, block_rows(0, j), :],
            dst_ref=retin.at[h, t, block_rows(0, j), :],
            send_sem=rt_send.at[t, h, j],
            recv_sem=rt_recv.at[t, h, j],
            device_id={"seq": lax.rem(s + NSEQ - ROW, NSEQ)},
            device_id_type=MESH,
        )

    outs = (dk_hbm, dv_hbm, dq_hbm)

    def out_src(t, h):
        return qout.at[h] if t == 2 else fin.at[h, t]

    def out_remote(t, h, j):
        lanes = pl.ds(pl.multiple_of((col * HPD + h) * HD, HD), HD)
        return pltpu.make_async_remote_copy(
            src_ref=out_src(t, h).at[block_rows(0, j), :],
            dst_ref=outs[t].at[0, :, lanes],
            send_sem=o_send.at[t, h, j],
            recv_sem=o_recv.at[t, h, col],
            device_id={"seq": base + j},
            device_id_type=MESH,
        )

    def out_local(t, h):
        lanes = pl.ds(pl.multiple_of((col * HPD + h) * HD, HD), HD)
        return pltpu.make_async_copy(
            out_src(t, h).at[block_rows(0, col), :], outs[t].at[0, :, lanes], o_loc.at[t, h]
        )

    def out_wait(t, h, peer):
        lanes = pl.ds(pl.multiple_of((peer * HPD + h) * HD, HD), HD)
        pltpu.make_async_remote_copy(
            src_ref=out_src(t, h).at[block_rows(0, col), :],
            dst_ref=outs[t].at[0, :, lanes],
            send_sem=o_send.at[t, h, peer],
            recv_sem=o_recv.at[t, h, peer],
            device_id={"seq": base + peer},
            device_id_type=MESH,
        ).wait_recv()

    def out_start(ts, h, j):
        @pl.when(j == col)
        def _():
            for t in ts:
                out_local(t, h).start()

        @pl.when(j != col)
        def _():
            for t in ts:
                out_remote(t, h, j).start()

    def attention(h, hooks):
        for t in range(4):
            in_local(t, h).wait()
        for t in range(2, 4):
            for off in range(1, ROW):
                in_wait(t, h, off)

        @pl.when(jnp.logical_not(first))
        def _():
            for j in range(ROW):
                for t in range(2):
                    fw_copy(t, h, j).wait_recv()

        @pl.when(first)
        def _():
            zeros = jnp.zeros((OWN, HD), BF16)
            ks[h, pl.ds(0, OWN), :] = zeros
            vs[h, pl.ds(0, OWN), :] = zeros

        acc[h] = jnp.zeros(acc.shape[1:], F32)
        key_pos = lax.broadcasted_iota(jnp.int32, (BLK, BLK), 0)
        qry_pos = lax.broadcasted_iota(jnp.int32, (BLK, BLK), 1)
        causal = key_pos <= qry_pos

        @pl.loop(0, ROW)
        def _(i):
            run_hooks(hooks, i)
            at = pl.multiple_of(i * BLK, BLK)
            qrows = pl.ds(at, BLK)
            krows = pl.ds(at, OWN + BLK)
            qb = qs[h, qrows, :]
            dob = dos[h, qrows, :]
            kb = ks[h, krows, :]
            vb = vs[h, krows, :]
            st = dot(kb, qb, NT)
            dpt = dot(vb, dob, NT)

            def bias(kt):
                return jnp.where(jnp.logical_and(first, i + kt < ROW), NEG, 0.0).astype(F32)

            parts = [jnp.where(causal, st[OWN:], st[:BLK] + bias(0))]
            for kt in range(1, ROW):
                parts.append(st[kt * BLK : (kt + 1) * BLK] + bias(kt))
            scores = jnp.concatenate(parts, 0)
            dp = jnp.concatenate([jnp.where(causal, dpt[OWN:], dpt[:BLK]), dpt[BLK:OWN]], 0)
            top = jnp.max(scores, axis=0, keepdims=True)
            raw = jnp.exp2((scores - top) * (SCALE * LOG2E))
            prob = raw * (1.0 / jnp.sum(raw, axis=0, keepdims=True))
            pb = prob.astype(BF16)
            delta = jnp.sum(pb.astype(F32) * dp, axis=0, keepdims=True)
            ds = prob * (dp - delta)
            zero = jnp.zeros((BLK, BLK), F32)
            pfull = jnp.concatenate(
                [jnp.where(causal, zero, prob[:BLK]).astype(BF16), pb[BLK:], jnp.where(causal, prob[:BLK], zero).astype(BF16)], 0
            )
            dsb = ds.astype(BF16)
            dfull = jnp.concatenate(
                [jnp.where(causal, zero, ds[:BLK]).astype(BF16), dsb[BLK:], jnp.where(causal, ds[:BLK], zero).astype(BF16)], 0
            )
            acc[h, 1, krows, :] += dot(pfull, dob, NN)
            acc[h, 0, krows, :] += dot(dfull, qb, NN)
            dq = dot(kb, dfull, TN)
            qout[h, qrows, :] = (dq.T * SCALE).astype(BF16)

            out_start((2,), h, i)

            @pl.when(jnp.logical_not(first))
            def _():
                retout[h, 0, qrows, :] = (acc[h, 0, qrows, :] * SCALE).astype(BF16)
                retout[h, 1, qrows, :] = acc[h, 1, qrows, :].astype(BF16)
                for t in range(2):
                    rt_copy(t, h, i).start()

    def finish_head(h):
        @pl.loop(0, ROW)
        def _(j):
            rows = block_rows(0, j)
            own = block_rows(OWN, j)
            for t in range(2):
                scale = SCALE if t == 0 else 1.0

                @pl.when(last)
                def _():
                    fin[h, t, rows, :] = (acc[h, t, own, :] * scale).astype(BF16)

                @pl.when(jnp.logical_not(last))
                def _():
                    rt_copy(t, h, j).wait_recv()
                    mine = acc[h, t, own, :] * scale
                    fin[h, t, rows, :] = (mine + retin[h, t, rows, :].astype(F32)).astype(BF16)

            out_start((0, 1), h, j)

    def drain():
        @pl.loop(0, HPD)
        def _(h):
            for t in range(4):
                for off in range(1, ROW):
                    in_copy(t, h, off).wait_send()

            @pl.loop(0, ROW)
            def _(j):
                for t in range(2):

                    @pl.when(jnp.logical_not(last))
                    def _():
                        fw_copy(t, h, j).wait_send()

                    @pl.when(jnp.logical_not(first))
                    def _():
                        rt_copy(t, h, j).wait_send()

                @pl.when(j == col)
                def _():
                    for t in range(3):
                        out_local(t, h).wait()

                @pl.when(j != col)
                def _():
                    for t in range(3):
                        out_remote(t, h, j).wait_send()
                        out_wait(t, h, j)

    def mixer_tables():
        bin32 = bin_ref[0].astype(F32)
        cout32 = cout_ref[0].astype(F32)
        for tab, rows32 in ((btab, bin32), (ctab, cout32)):
            for n in range(NST):
                wide = jnp.broadcast_to(rows32[n : n + 1, :], (TOK, TOK)).T
                for k in range(NCH):
                    natt[pl.ds(k * PITCH, LEN), :] = wide[k * LEN : (k + 1) * LEN]
                for j in range(LEN):
                    tab[n, j] = natt[pl.ds(j, NCH, stride=PITCH), :]

    def spread(block, n):
        return jnp.broadcast_to(block[n : n + 1, :], (NCH, 128))

    def mixer_local(c):
        lanes = pl.ds(pl.multiple_of(c * 128, 128), 128)
        x = x_ref[0, :, lanes].astype(F32)
        z = raw_ref[0, :, lanes].astype(F32) + bias_ref[:, lanes]
        ct = cot_ref[0, :, lanes].astype(F32)
        small = jnp.exp(-jnp.abs(z))
        dt = jnp.maximum(z, 0.0) + jnp.log1p(small)
        sg = jnp.where(z >= 0.0, 1.0, small) / (1.0 + small)
        par[c, 9:10, :] = jnp.sum(ct * x, axis=0, keepdims=True)
        for k in range(NCH):
            rows = pl.ds(k * PITCH, LEN)
            part = slice(k * LEN, (k + 1) * LEN)
            dts[c, rows, :] = dt[part]
            xs[c, rows, :] = x[part]
            cts[c, rows, :] = ct[part]
            sgs[c, rows, :] = sg[part]
        a2 = -jnp.exp(dl_ref[:, lanes]) * LOG2E
        a2s[c] = a2
        rate = [spread(a2, n) for n in range(NST)]
        state = [jnp.zeros((NCH, 128), F32) for _ in range(NST)]
        decay = [jnp.ones((NCH, 128), F32) for _ in range(NST)]
        back = [jnp.zeros((NCH, 128), F32) for _ in range(NST)]
        for j in range(LEN):
            rows = pl.ds(j, NCH, stride=PITCH)
            dtj = dts[c, rows, :]
            uj = dtj * xs[c, rows, :]
            cj = cts[c, rows, :]
            for n in range(NST):
                a = jnp.exp2(dtj * rate[n])
                avs[c, j, n] = a
                state[n] = a * state[n] + uj * btab[n, j]
                decay[n] = a * decay[n]
                back[n] = back[n] + decay[n] * (cj * ctab[n, j])
        for n in range(NST):
            rows = pl.ds(n * NCH, NCH)
            tscr[0, rows, :] = state[n]
            tscr[1, rows, :] = decay[n]
            tscr[2, rows, :] = back[n]
        ek = [tscr[0, pl.ds(k, NST, stride=NCH), :] for k in range(NCH)]
        dk = [tscr[1, pl.ds(k, NST, stride=NCH), :] for k in range(NCH)]
        bk = [tscr[2, pl.ds(k, NST, stride=NCH), :] for k in range(NCH)]
        pd = jnp.ones((NST, 128), F32)
        pe = jnp.zeros((NST, 128), F32)
        for k in range(NCH):
            pds[c, k] = pd
            pes[c, k] = pe
            pe = dk[k] * pe + ek[k]
            pd = dk[k] * pd
        sd = jnp.ones((NST, 128), F32)
        sb = jnp.zeros((NST, 128), F32)
        for k in reversed(range(NCH)):
            sds[c, k] = sd
            sbs[c, k] = sb
            sb = dk[k] * sb + bk[k]
            sd = dk[k] * sd
        tot[c, 0:8, :] = pe
        tot[c, 8:16, :] = pd
        tot[c, 16:24, :] = sb

    def scatter(src, dst, send, recv):
        @pl.loop(0, TILES)
        def _(j):
            @pl.when(j != s)
            def _():
                pltpu.make_async_remote_copy(
                    src_ref=src.at[j], dst_ref=dst.at[s], send_sem=send, recv_sem=recv,
                    device_id={"seq": j}, device_id_type=MESH,
                ).start()

        @pl.when(s < TILES)
        def _():
            dst[s] = src[s]

    def scatter_wait_recv(dst, sem):
        head = dst.at[pl.ds(0, NSEQ - 1)]
        pltpu.make_async_copy(head, head, sem).wait()

    def tiles_wait(ref, sem):
        @pl.when(s < TILES)
        def _():
            part = ref.at[pl.ds(0, TILES - 1)]
            pltpu.make_async_copy(part, part, sem).wait()

        @pl.when(s >= TILES)
        def _():
            part = ref.at[pl.ds(0, TILES)]
            pltpu.make_async_copy(part, part, sem).wait()

    def spread_out(src_of, dst, send, recv):
        @pl.loop(0, NSEQ)
        def _(i):
            @pl.when(i != s)
            def _():
                pltpu.make_async_remote_copy(
                    src_ref=src_of(i), dst_ref=dst.at[s], send_sem=send, recv_sem=recv,
                    device_id={"seq": i}, device_id_type=MESH,
                ).start()

    def mixer_prefix():
        @pl.when(s < TILES)
        def _():
            scatter_wait_recv(gath, a_recv)
            carry = jnp.zeros((NST, 128), F32)
            for i in range(NSEQ):
                cbuf[i, 0:8, :] = carry
                carry = gath[i, 8:16, :] * carry + gath[i, 0:8, :]
            carry = jnp.zeros((NST, 128), F32)
            for i in reversed(range(NSEQ)):
                cbuf[i, 8:16, :] = carry
                carry = gath[i, 8:16, :] * carry + gath[i, 16:24, :]
            spread_out(lambda i: cbuf.at[i], cin, b_send, b_recv)
            cin[s] = cbuf[s]

    def mixer_back(c):
        lanes = pl.ds(pl.multiple_of(c * 128, 128), 128)
        hin = cin[c, 0:8, :]
        gin = cin[c, 8:16, :]
        for k in range(NCH):
            rows = pl.ds(k * NST, NST)
            tscr[0, rows, :] = pds[c, k] * hin + pes[c, k]
            tscr[1, rows, :] = sds[c, k] * gin + sbs[c, k]
        state = [tscr[0, pl.ds(n, NCH, stride=NST), :] for n in range(NST)]
        a2 = a2s[c]
        for j in range(LEN):
            rows = pl.ds(j, NCH, stride=PITCH)
            uj = dts[c, rows, :] * xs[c, rows, :]
            cj = cts[c, rows, :]
            for n in range(NST):
                ah = avs[c, j, n] * state[n]
                ahs[j, n] = ah
                state[n] = ah + uj * btab[n, j]
                gcacc[n, pl.ds(j * NCH, NCH), :] += cj * state[n]
        adj = [tscr[1, pl.ds(n, NCH, stride=NST), :] for n in range(NST)]
        ga = [jnp.zeros((NCH, 128), F32) for _ in range(NST)]
        rate = [spread(a2, n) for n in range(NST)]
        skip = jnp.broadcast_to(skip_ref[:, lanes], (NCH, 128))
        gb = jnp.zeros((NCH, 128), F32)
        for j in reversed(range(LEN)):
            rows = pl.ds(j, NCH, stride=PITCH)
            dtj = dts[c, rows, :]
            xj = xs[c, rows, :]
            uj = dtj * xj
            cj = cts[c, rows, :]
            proj = None
            gdt = None
            for n in range(NST):
                gn = adj[n] + ctab[n, j] * cj
                gbacc[n, pl.ds(j * NCH, NCH), :] += gn * uj
                w = gn * ahs[j, n]
                ga[n] = ga[n] + w * dtj
                p1 = gn * btab[n, j]
                p2 = w * rate[n]
                proj = p1 if proj is None else proj + p1
                gdt = p2 if gdt is None else gdt + p2
                adj[n] = avs[c, j, n] * gn
            gxt[rows, :] = skip * cj + dtj * proj
            graw = (xj * proj + gdt * LN2) * sgs[c, rows, :]
            grt[rows, :] = graw
            gb = gb + graw
        for n in range(NST):
            tscr[2, pl.ds(n * NCH, NCH), :] = ga[n]
        gsum = tscr[2, pl.ds(0, NST, stride=NCH), :]
        for k in range(1, NCH):
            gsum = gsum + tscr[2, pl.ds(k, NST, stride=NCH), :]
        par[c, 0:8, :] = gsum * (a2 * LN2)
        par[c, 8:9, :] = jnp.sum(gb, axis=0, keepdims=True)
        for k in range(NCH):
            rows = pl.ds(k * PITCH, LEN)
            gx_ref[0, pl.ds(k * LEN, LEN), lanes] = gxt[rows, :].astype(BF16)
            gr_ref[0, pl.ds(k * LEN, LEN), lanes] = grt[rows, :].astype(BF16)

    def mixer_state_grads():
        ones = jnp.ones((8, 128), F32)
        for accum, ref in ((gbacc, gin_ref), (gcacc, gout_ref)):
            for n in range(NST):
                rows = [accum[n, pl.ds(k, LEN, stride=NCH), :] for k in range(NCH)]
                full = jnp.concatenate(rows, 0)
                line = lax.dot_general(
                    ones, full, NT, preferred_element_type=F32, precision=lax.Precision.HIGHEST
                )
                gred[n : n + 1, :] = line[0:1, :]
            ref[0] = gred[...].astype(BF16)

    def params_rows():
        @pl.when(s < TILES)
        def _():
            scatter_wait_recv(pgat, c_recv)
            total = pgat[0]
            for i in range(1, NSEQ):
                total = total + pgat[i]
            psm[...] = total
            p4[g] = total

            @pl.loop(0, NGRP)
            def _(i):
                @pl.when(i != g)
                def _():
                    pltpu.make_async_remote_copy(
                        src_ref=psm, dst_ref=p4.at[g], send_sem=d_send, recv_sem=d_recv,
                        device_id={"grp": i}, device_id_type=MESH,
                    ).start()

    def params_groups():
        @pl.when(s < TILES)
        def _():
            head = p4.at[pl.ds(0, NGRP - 1)]
            pltpu.make_async_copy(head, head, d_recv).wait()
            final = (p4[0] + p4[1]) + (p4[2] + p4[3])
            pfin[...] = final
            pout[s] = final
            spread_out(lambda i: pfin, pout, e_send, e_recv)

    def params_store():
        tiles_wait(pout, e_recv)

        @pl.loop(0, TILES)
        def _(c):
            lanes = pl.ds(pl.multiple_of(c * 128, 128), 128)
            gdec_ref[:, lanes] = pout[c, 0:8, :]
            gbias_ref[:, lanes] = pout[c, 8:9, :]
            gskip_ref[:, lanes] = pout[c, 9:10, :]

    def mixer_drain():
        tiles_wait(tot, a_send)
        tiles_wait(par, c_send)

        @pl.when(s < TILES)
        def _():
            part = cbuf.at[pl.ds(0, NSEQ - 1)]
            pltpu.make_async_copy(part, part, b_send).wait()
            part = p4.at[pl.ds(0, NGRP - 1)]
            pltpu.make_async_copy(part, part, d_send).wait()
            part = pgat.at[pl.ds(0, NSEQ - 1)]
            pltpu.make_async_copy(part, part, e_send).wait()

    def run_hooks(hooks, i):
        for at, action in hooks:

            @pl.when(i == at)
            def _():
                action()

    def tiles(body, start, stop, hooks):
        @pl.loop(start, stop)
        def _(c):
            run_hooks(hooks, c)
            body(c)

    K, VV, Q, DO = range(4)

    def send(*pairs):
        def go():
            for t, h in pairs:
                send_in(t, h)

        return go

    send((K, 0), (VV, 0))()
    for h in range(HPD):
        forward_own(h)
    mixer_tables()
    tiles(mixer_local, 0, TILES, [(4, send((Q, 0))), (16, lambda: forward_rest(0))])
    scatter(tot, gath, a_send, a_recv)
    send((DO, 0), (K, 1), (VV, 1))()
    gbacc[...] = jnp.zeros(gbacc.shape, F32)
    gcacc[...] = jnp.zeros(gcacc.shape, F32)
    par[:, 10:16, :] = jnp.zeros((TILES, 6, 128), F32)
    mixer_prefix()
    send((Q, 1), (DO, 1))()
    attention(0, [(2, lambda: forward_rest(1)), (3, send((K, 2), (VV, 2)))])
    tiles_wait(cin, b_recv)
    tiles(mixer_back, 0, TILES // 2, [(1, send((Q, 2), (DO, 2))), (TILES // 2 - 3, lambda: forward_rest(2))])
    attention(1, [])
    finish_head(0)
    tiles(mixer_back, TILES // 2, TILES, [])
    scatter(par, pgat, c_send, c_recv)
    attention(2, [])
    params_rows()
    mixer_state_grads()
    finish_head(1)
    params_groups()
    finish_head(2)
    params_store()
    mixer_drain()
    drain()


def store_results(*refs):
    n = len(refs) // 2
    srcs, outs, sems = refs[:n], refs[n : 2 * n], refs[2 * n]
    copies = [pltpu.make_async_copy(a, b, sems.at[i]) for i, (a, b) in enumerate(zip(srcs, outs))]
    for copy in copies:
        copy.start()
    for copy in copies:
        copy.wait()


def per_device(queries, keys, values, cot_attn, x, raw, bin_, cout, cot, decay_log, step_bias, skip_gain):
    vm = pl.BlockSpec(memory_space=pltpu.VMEM)
    hbm = pl.BlockSpec(memory_space=pl.ANY)
    att = jax.ShapeDtypeStruct((1, BLK, 12 * HD), BF16)
    mix = jax.ShapeDtypeStruct((1, TOK, INNER), BF16)
    stt = jax.ShapeDtypeStruct((1, NST, TOK), BF16)
    chan = jax.ShapeDtypeStruct((1, INNER), F32)
    V = pltpu.VMEM
    shapes = (att, att, att, mix, mix, stt, stt, jax.ShapeDtypeStruct((NST, INNER), F32), chan, chan)
    D = pltpu.SemaphoreType.DMA
    scratch = [
        V((HPD, OWN, HD), BF16), V((HPD, OWN, HD), BF16), V((HPD, 2 * OWN, HD), BF16), V((HPD, 2 * OWN, HD), BF16),
        V((HPD, 2, 2 * OWN, HD), F32), V((HPD, OWN, HD), BF16),
        V((HPD, 2, OWN, HD), BF16), V((HPD, 2, OWN, HD), BF16), V((HPD, 2, OWN, HD), BF16),
        *[V((TILES, NCH * PITCH, 128), F32)] * 4,
        V((TILES, LEN, NST, NCH, 128), F32), V((TILES, NST, 128), F32),
        V((NST, LEN, NCH, 128), F32), V((NST, LEN, NCH, 128), F32), V((NCH * PITCH, 128), F32),
        V((3, NST * NCH, 128), F32),
        *[V((TILES, NCH, NST, 128), F32)] * 4,
        V((TILES, 24, 128), F32), V((NSEQ, 24, 128), F32), V((NSEQ, 16, 128), F32), V((TILES, 16, 128), F32),
        V((LEN, NST, NCH, 128), F32), V((NCH * PITCH, 128), F32), V((NCH * PITCH, 128), F32),
        V((NST, LEN * NCH, 128), F32), V((NST, LEN * NCH, 128), F32), V((NST, 128), F32),
        V((TILES, 16, 128), F32), V((NSEQ, 16, 128), F32), V((16, 128), F32), V((NGRP, 16, 128), F32),
        V((16, 128), F32), V((TILES, 16, 128), F32),
        D((4, HPD, ROW - 1)), D((4, HPD, ROW - 1)), D((4, HPD)),
        *[D((2, HPD, ROW))] * 4,
        D((3, HPD, ROW)), D((3, HPD, ROW)), D((3, HPD)),
        *[D(())] * 10,
    ]
    res = pl.pallas_call(
        kernel,
        out_shape=tuple(V(a.shape, a.dtype) for a in shapes),
        in_specs=[hbm] * 4 + [vm] * 8,
        out_specs=(vm,) * 10,
        scratch_shapes=scratch,
        compiler_params=pltpu.CompilerParams(
            collective_id=0, has_side_effects=True, vmem_limit_bytes=56 * 1024 * 1024
        ),
    )(queries, keys, values, cot_attn, x, raw, bin_, cout, cot, decay_log, step_bias.reshape(1, -1), skip_gain.reshape(1, -1))
    res = pl.pallas_call(
        store_results,
        out_shape=shapes,
        in_specs=[vm] * len(shapes),
        out_specs=(hbm,) * len(shapes),
        scratch_shapes=[D((len(shapes),))],
        compiler_params=pltpu.CompilerParams(vmem_limit_bytes=4 * 1024 * 1024),
    )(*[pltpu.with_memory_space_constraint(a, pltpu.VMEM) for a in res])
    return tuple(res[:8]) + (res[8].reshape(-1), res[9].reshape(-1))


def solution(mesh):
    tok = P("grp", "seq", None)
    stt = P("grp", None, "seq")
    return jax.shard_map(
        per_device,
        mesh=mesh,
        in_specs=(tok,) * 4 + (tok, tok, stt, stt, tok, P(), P(), P()),
        out_specs=(tok,) * 3 + (tok, tok, stt, stt, P(), P(), P()),
        check_vma=False,
    )
```

```python
import functools

import jax
import jax.numpy as jnp
from jax import lax
from jax.experimental import pallas as pl
from jax.experimental.pallas import tpu as pltpu
from jax.sharding import PartitionSpec as P

MESH = pl.DeviceIdType.MESH
F32 = jnp.float32
BF16 = jnp.bfloat16

NSEQ = 32
NGRP = 4
ROW = 4
NROW = NSEQ // ROW
BLK = 256
OWN = ROW * BLK
HPD = 3
HD = 128
TOK = 128
NCH = 8
LEN = TOK // NCH
PITCH = 24
NST = 8
TILES = 24
INNER = TILES * 128
LOG2E = 1.4426950408889634
LN2 = 0.6931471805599453
NEG = -1e30
SCALE = HD**-0.5

NT = (((1,), (1,)), ((), ()))
NN = (((1,), (0,)), ((), ()))
TN = (((0,), (0,)), ((), ()))


def dot(a, b, dims):
    return lax.dot_general(a, b, dims, preferred_element_type=F32)


def kernel(
    q_hbm, k_hbm, v_hbm, do_hbm, x_hbm, raw_hbm, bin_ref, cout_ref, cot_hbm, dl_ref, bias_ref, skip_ref,
    dq_hbm, dk_hbm, dv_hbm, gx_ref, gr_ref, gin_ref, gout_ref, gdec_ref, gbias_ref, gskip_ref,
    qs, dos, ks, vs, acc, qout, retout, retin, fin,
    x_ref, raw_ref, cot_ref, mix_sem, dts, xs, cts, sgs, avs, a2s, btab, ctab, natt, tscr, pds, pes, sds, sbs, tot, dtot, gath, gdt, ahead, cbuf, cin,
    ahs, gxt, grt, gbacc, gcacc, gred, par, pgat, psm, p4, pfin, pout,
    in_send, in_recv, in_loc, fw_send, fw_recv, rt_send, rt_recv, o_send, o_recv, o_loc,
    a_send, a_recv, t_send, t_recv, b_send, b_recv, c_send, c_recv, d_send, d_recv, e_send, e_recv,
):
    s = lax.axis_index("seq")
    g = lax.axis_index("grp")
    col = lax.rem(s, ROW)
    base = s - col
    row = s // ROW
    first = row == 0
    last = row == NROW - 1

    mix_in = [
        pltpu.make_async_copy(src, dst, mix_sem.at[i])
        for i, (src, dst) in enumerate(((x_hbm, x_ref), (raw_hbm, raw_ref), (cot_hbm, cot_ref)))
    ]
    for copy in mix_in:
        copy.start()

    barrier = pltpu.get_barrier_semaphore()

    @pl.loop(0, NSEQ)
    def _(i):
        @pl.when(i != s)
        def _():
            pl.semaphore_signal(barrier, inc=1, device_id={"seq": i}, device_id_type=MESH)

    @pl.loop(0, NGRP)
    def _(i):
        @pl.when(i != g)
        def _():
            pl.semaphore_signal(barrier, inc=1, device_id={"grp": i}, device_id_type=MESH)

    pl.semaphore_wait(barrier, NSEQ + NGRP - 2)

    srcs = (k_hbm, v_hbm, q_hbm, do_hbm)
    dsts = (ks, vs, qs, dos)
    lead = (OWN, OWN, 0, 0)

    def in_copy(t, h, off):
        peer = lax.rem(col + off, ROW)
        lanes = pl.ds(pl.multiple_of((peer * HPD + h) * HD, HD), HD)
        rows = pl.ds(pl.multiple_of(lead[t] + col * BLK, BLK), BLK)
        return pltpu.make_async_remote_copy(
            src_ref=srcs[t].at[0, :, lanes],
            dst_ref=dsts[t].at[h, rows, :],
            send_sem=in_send.at[t, h, off - 1],
            recv_sem=in_recv.at[t, h, off - 1],
            device_id={"seq": base + peer},
            device_id_type=MESH,
        )

    def in_wait(t, h, off):
        peer = lax.rem(col + ROW - off, ROW)
        lanes = pl.ds(pl.multiple_of((col * HPD + h) * HD, HD), HD)
        rows = pl.ds(pl.multiple_of(lead[t] + peer * BLK, BLK), BLK)
        pltpu.make_async_remote_copy(
            src_ref=srcs[t].at[0, :, lanes],
            dst_ref=dsts[t].at[h, rows, :],
            send_sem=in_send.at[t, h, off - 1],
            recv_sem=in_recv.at[t, h, off - 1],
            device_id={"seq": base + peer},
            device_id_type=MESH,
        ).wait_recv()

    def in_local(t, h):
        lanes = pl.ds(pl.multiple_of((col * HPD + h) * HD, HD), HD)
        rows = pl.ds(pl.multiple_of(lead[t] + col * BLK, BLK), BLK)
        return pltpu.make_async_copy(
            srcs[t].at[0, :, lanes], dsts[t].at[h, rows, :], in_loc.at[t, h]
        )

    def send_in(t, h):
        for off in range(1, ROW):
            in_copy(t, h, off).start()
        in_local(t, h).start()

    def block_rows(start, j):
        return pl.ds(pl.multiple_of(start + j * BLK, BLK), BLK)

    def fw_copy(t, h, j, own=False):
        lanes = pl.ds(pl.multiple_of((col * HPD + h) * HD, HD), HD)
        return pltpu.make_async_remote_copy(
            src_ref=srcs[t].at[0, :, lanes] if own else dsts[t].at[h, block_rows(OWN, j), :],
            dst_ref=dsts[t].at[h, block_rows(0, j), :],
            send_sem=fw_send.at[t, h, j],
            recv_sem=fw_recv.at[t, h, j],
            device_id={"seq": lax.rem(s + ROW, NSEQ)},
            device_id_type=MESH,
        )

    def forward_own(h):
        @pl.when(jnp.logical_not(last))
        def _():
            for t in range(2):
                fw_copy(t, h, col, own=True).start()

    def forward_rest(h):
        for off in range(1, ROW):
            for t in range(2):
                in_wait(t, h, off)

            @pl.when(jnp.logical_not(last))
            def _():
                for t in range(2):
                    fw_copy(t, h, lax.rem(col + ROW - off, ROW)).start()

    def rt_copy(t, h, j):
        return pltpu.make_async_remote_copy(
            src_ref=retout.at[h, t, block_rows(0, j), :],
            dst_ref=retin.at[h, t, block_rows(0, j), :],
            send_sem=rt_send.at[t, h, j],
            recv_sem=rt_recv.at[t, h, j],
            device_id={"seq": lax.rem(s + NSEQ - ROW, NSEQ)},
            device_id_type=MESH,
        )

    outs = (dk_hbm, dv_hbm, dq_hbm)

    def out_src(t, h):
        return qout.at[h] if t == 2 else fin.at[h, t]

    def out_remote(t, h, j):
        lanes = pl.ds(pl.multiple_of((col * HPD + h) * HD, HD), HD)
        return pltpu.make_async_remote_copy(
            src_ref=out_src(t, h).at[block_rows(0, j), :],
            dst_ref=outs[t].at[0, :, lanes],
            send_sem=o_send.at[t, h, j],
            recv_sem=o_recv.at[t, h, col],
            device_id={"seq": base + j},
            device_id_type=MESH,
        )

    def out_local(t, h):
        lanes = pl.ds(pl.multiple_of((col * HPD + h) * HD, HD), HD)
        return pltpu.make_async_copy(
            out_src(t, h).at[block_rows(0, col), :], outs[t].at[0, :, lanes], o_loc.at[t, h]
        )

    def out_wait(t, h, peer):
        lanes = pl.ds(pl.multiple_of((peer * HPD + h) * HD, HD), HD)
        pltpu.make_async_remote_copy(
            src_ref=out_src(t, h).at[block_rows(0, col), :],
            dst_ref=outs[t].at[0, :, lanes],
            send_sem=o_send.at[t, h, peer],
            recv_sem=o_recv.at[t, h, peer],
            device_id={"seq": base + peer},
            device_id_type=MESH,
        ).wait_recv()

    def out_start(ts, h, j):
        @pl.when(j == col)
        def _():
            for t in ts:
                out_local(t, h).start()

        @pl.when(j != col)
        def _():
            for t in ts:
                out_remote(t, h, j).start()

    def attention(h, hooks):
        for t in range(4):
            in_local(t, h).wait()
        for t in range(2, 4):
            for off in range(1, ROW):
                in_wait(t, h, off)

        @pl.when(jnp.logical_not(first))
        def _():
            for j in range(ROW):
                for t in range(2):
                    fw_copy(t, h, j).wait_recv()

        @pl.when(first)
        def _():
            zeros = jnp.zeros((OWN, HD), BF16)
            ks[h, pl.ds(0, OWN), :] = zeros
            vs[h, pl.ds(0, OWN), :] = zeros

        acc[h] = jnp.zeros(acc.shape[1:], F32)
        key_pos = lax.broadcasted_iota(jnp.int32, (BLK, BLK), 0)
        qry_pos = lax.broadcasted_iota(jnp.int32, (BLK, BLK), 1)
        causal = key_pos <= qry_pos

        @pl.loop(0, ROW)
        def _(i):
            run_hooks(hooks, i)
            at = pl.multiple_of(i * BLK, BLK)
            qrows = pl.ds(at, BLK)
            krows = pl.ds(at, OWN + BLK)
            qb = qs[h, qrows, :]
            dob = dos[h, qrows, :]
            kb = ks[h, krows, :]
            vb = vs[h, krows, :]
            st = dot(kb, qb, NT)
            dpt = dot(vb, dob, NT)

            def bias(kt):
                return jnp.where(jnp.logical_and(first, i + kt < ROW), NEG, 0.0).astype(F32)

            parts = [jnp.where(causal, st[OWN:], st[:BLK] + bias(0))]
            for kt in range(1, ROW):
                parts.append(st[kt * BLK : (kt + 1) * BLK] + bias(kt))
            scores = jnp.concatenate(parts, 0)
            dp = jnp.concatenate([jnp.where(causal, dpt[OWN:], dpt[:BLK]), dpt[BLK:OWN]], 0)
            top = jnp.max(scores, axis=0, keepdims=True)
            raw = jnp.exp2((scores - top) * (SCALE * LOG2E))
            prob = raw * (1.0 / jnp.sum(raw, axis=0, keepdims=True))
            pb = prob.astype(BF16)
            delta = jnp.sum(pb.astype(F32) * dp, axis=0, keepdims=True)
            ds = prob * (dp - delta)
            zero = jnp.zeros((BLK, BLK), F32)
            pfull = jnp.concatenate(
                [jnp.where(causal, zero, prob[:BLK]).astype(BF16), pb[BLK:], jnp.where(causal, prob[:BLK], zero).astype(BF16)], 0
            )
            dsb = ds.astype(BF16)
            dfull = jnp.concatenate(
                [jnp.where(causal, zero, ds[:BLK]).astype(BF16), dsb[BLK:], jnp.where(causal, ds[:BLK], zero).astype(BF16)], 0
            )
            acc[h, 1, krows, :] += dot(pfull, dob, NN)
            acc[h, 0, krows, :] += dot(dfull, qb, NN)
            dq = dot(kb, dfull, TN)
            qout[h, qrows, :] = (dq.T * SCALE).astype(BF16)

            out_start((2,), h, i)

            @pl.when(jnp.logical_not(first))
            def _():
                retout[h, 0, qrows, :] = (acc[h, 0, qrows, :] * SCALE).astype(BF16)
                retout[h, 1, qrows, :] = acc[h, 1, qrows, :].astype(BF16)
                for t in range(2):
                    rt_copy(t, h, i).start()

    def finish_head(h):
        @pl.loop(0, ROW)
        def _(j):
            rows = block_rows(0, j)
            own = block_rows(OWN, j)
            for t in range(2):
                scale = SCALE if t == 0 else 1.0

                @pl.when(last)
                def _():
                    fin[h, t, rows, :] = (acc[h, t, own, :] * scale).astype(BF16)

                @pl.when(jnp.logical_not(last))
                def _():
                    rt_copy(t, h, j).wait_recv()
                    mine = acc[h, t, own, :] * scale
                    fin[h, t, rows, :] = (mine + retin[h, t, rows, :].astype(F32)).astype(BF16)

            out_start((0, 1), h, j)

    def drain():
        @pl.loop(0, HPD)
        def _(h):
            for t in range(4):
                for off in range(1, ROW):
                    in_copy(t, h, off).wait_send()

            @pl.loop(0, ROW)
            def _(j):
                for t in range(2):

                    @pl.when(jnp.logical_not(last))
                    def _():
                        fw_copy(t, h, j).wait_send()

                    @pl.when(jnp.logical_not(first))
                    def _():
                        rt_copy(t, h, j).wait_send()

                @pl.when(j == col)
                def _():
                    for t in range(3):
                        out_local(t, h).wait()

                @pl.when(j != col)
                def _():
                    for t in range(3):
                        out_remote(t, h, j).wait_send()
                        out_wait(t, h, j)

    def mixer_tables():
        bin32 = bin_ref[0].astype(F32)
        cout32 = cout_ref[0].astype(F32)
        for tab, rows32 in ((btab, bin32), (ctab, cout32)):
            for n in range(NST):
                wide = jnp.broadcast_to(rows32[n : n + 1, :], (TOK, TOK)).T
                for k in range(NCH):
                    natt[pl.ds(k * PITCH, LEN), :] = wide[k * LEN : (k + 1) * LEN]
                for j in range(LEN):
                    tab[n, j] = natt[pl.ds(j, NCH, stride=PITCH), :]

    def spread(block, n):
        return jnp.broadcast_to(block[n : n + 1, :], (NCH, 128))

    def mixer_local(c):
        lanes = pl.ds(pl.multiple_of(c * 128, 128), 128)
        x = x_ref[0, :, lanes].astype(F32)
        z = raw_ref[0, :, lanes].astype(F32) + bias_ref[:, lanes]
        ct = cot_ref[0, :, lanes].astype(F32)
        small = jnp.exp(-jnp.abs(z))
        dt = jnp.maximum(z, 0.0) + jnp.log1p(small)
        sg = jnp.where(z >= 0.0, 1.0, small) / (1.0 + small)
        par[c, 9:10, :] = jnp.sum(ct * x, axis=0, keepdims=True)
        for k in range(NCH):
            rows = pl.ds(k * PITCH, LEN)
            part = slice(k * LEN, (k + 1) * LEN)
            dts[c, rows, :] = dt[part]
            xs[c, rows, :] = x[part]
            cts[c, rows, :] = ct[part]
            sgs[c, rows, :] = sg[part]
        a2 = -jnp.exp(dl_ref[:, lanes]) * LOG2E
        a2s[c] = a2
        rate = [spread(a2, n) for n in range(NST)]
        state = [jnp.zeros((NCH, 128), F32) for _ in range(NST)]
        decay = [jnp.ones((NCH, 128), F32) for _ in range(NST)]
        back = [jnp.zeros((NCH, 128), F32) for _ in range(NST)]
        for j in range(LEN):
            rows = pl.ds(j, NCH, stride=PITCH)
            dtj = dts[c, rows, :]
            uj = dtj * xs[c, rows, :]
            cj = cts[c, rows, :]
            for n in range(NST):
                a = jnp.exp2(dtj * rate[n])
                avs[c, j, n] = a
                state[n] = a * state[n] + uj * btab[n, j]
                decay[n] = a * decay[n]
                back[n] = back[n] + decay[n] * (cj * ctab[n, j])
        for n in range(NST):
            rows = pl.ds(n * NCH, NCH)
            tscr[0, rows, :] = state[n]
            tscr[1, rows, :] = decay[n]
            tscr[2, rows, :] = back[n]
        ek = [tscr[0, pl.ds(k, NST, stride=NCH), :] for k in range(NCH)]
        dk = [tscr[1, pl.ds(k, NST, stride=NCH), :] for k in range(NCH)]
        bk = [tscr[2, pl.ds(k, NST, stride=NCH), :] for k in range(NCH)]
        pd = jnp.ones((NST, 128), F32)
        pe = jnp.zeros((NST, 128), F32)
        for k in range(NCH):
            pds[c, k] = pd
            pes[c, k] = pe
            pe = dk[k] * pe + ek[k]
            pd = dk[k] * pd
        sd = jnp.ones((NST, 128), F32)
        sb = jnp.zeros((NST, 128), F32)
        for k in reversed(range(NCH)):
            sds[c, k] = sd
            sbs[c, k] = sb
            sb = dk[k] * sb + bk[k]
            sd = dk[k] * sd
        tot[c] = jnp.concatenate([pe, sb], 0).astype(BF16)
        dtot[c] = jnp.sum(dt, axis=0, keepdims=True)

    def scatter(src, dst, send, recv):
        @pl.loop(0, TILES)
        def _(j):
            @pl.when(j != s)
            def _():
                pltpu.make_async_remote_copy(
                    src_ref=src.at[j], dst_ref=dst.at[s], send_sem=send, recv_sem=recv,
                    device_id={"seq": j}, device_id_type=MESH,
                ).start()

        @pl.when(s < TILES)
        def _():
            dst[s] = src[s]

    def scatter_wait_recv(dst, sem):
        head = dst.at[pl.ds(0, NSEQ - 1)]
        pltpu.make_async_copy(head, head, sem).wait()

    def tiles_wait(ref, sem):
        @pl.when(s < TILES)
        def _():
            part = ref.at[pl.ds(0, TILES - 1)]
            pltpu.make_async_copy(part, part, sem).wait()

        @pl.when(s >= TILES)
        def _():
            part = ref.at[pl.ds(0, TILES)]
            pltpu.make_async_copy(part, part, sem).wait()

    def spread_out(src_of, dst, send, recv):
        @pl.loop(0, NSEQ)
        def _(i):
            @pl.when(i != s)
            def _():
                pltpu.make_async_remote_copy(
                    src_ref=src_of(i), dst_ref=dst.at[s], send_sem=send, recv_sem=recv,
                    device_id={"seq": i}, device_id_type=MESH,
                ).start()

    def mixer_prefix():
        @pl.when(s < TILES)
        def _():
            scatter_wait_recv(gath, a_recv)
            scatter_wait_recv(gdt, t_recv)
            a2 = a2s[s]
            carry = jnp.zeros((NST, 128), F32)
            for i in range(NSEQ):
                ahead[i] = carry
                carry = jnp.exp2(a2 * gdt[i]) * carry + gath[i].astype(F32)[0:8]
            carry = jnp.zeros((NST, 128), F32)
            for i in reversed(range(NSEQ)):
                cbuf[i] = jnp.concatenate([ahead[i], carry], 0).astype(BF16)
                carry = jnp.exp2(a2 * gdt[i]) * carry + gath[i].astype(F32)[8:16]
            spread_out(lambda i: cbuf.at[i], cin, b_send, b_recv)
            cin[s] = cbuf[s]

    def mixer_back(c):
        lanes = pl.ds(pl.multiple_of(c * 128, 128), 128)
        entering = cin[c].astype(F32)
        hin = entering[0:8]
        gin = entering[8:16]
        for k in range(NCH):
            rows = pl.ds(k * NST, NST)
            tscr[0, rows, :] = pds[c, k] * hin + pes[c, k]
            tscr[1, rows, :] = sds[c, k] * gin + sbs[c, k]
        state = [tscr[0, pl.ds(n, NCH, stride=NST), :] for n in range(NST)]
        a2 = a2s[c]
        for j in range(LEN):
            rows = pl.ds(j, NCH, stride=PITCH)
            uj = dts[c, rows, :] * xs[c, rows, :]
            cj = cts[c, rows, :]
            for n in range(NST):
                ah = avs[c, j, n] * state[n]
                ahs[j, n] = ah
                state[n] = ah + uj * btab[n, j]
                gcacc[n, pl.ds(j * NCH, NCH), :] += cj * state[n]
        adj = [tscr[1, pl.ds(n, NCH, stride=NST), :] for n in range(NST)]
        ga = [jnp.zeros((NCH, 128), F32) for _ in range(NST)]
        rate = [spread(a2, n) for n in range(NST)]
        skip = jnp.broadcast_to(skip_ref[:, lanes], (NCH, 128))
        gb = jnp.zeros((NCH, 128), F32)
        for j in reversed(range(LEN)):
            rows = pl.ds(j, NCH, stride=PITCH)
            dtj = dts[c, rows, :]
            xj = xs[c, rows, :]
            uj = dtj * xj
            cj = cts[c, rows, :]
            proj = None
            gdt = None
            for n in range(NST):
                gn = adj[n] + ctab[n, j] * cj
                gbacc[n, pl.ds(j * NCH, NCH), :] += gn * uj
                w = gn * ahs[j, n]
                ga[n] = ga[n] + w * dtj
                p1 = gn * btab[n, j]
                p2 = w * rate[n]
                proj = p1 if proj is None else proj + p1
                gdt = p2 if gdt is None else gdt + p2
                adj[n] = avs[c, j, n] * gn
            gxt[rows, :] = skip * cj + dtj * proj
            graw = (xj * proj + gdt * LN2) * sgs[c, rows, :]
            grt[rows, :] = graw
            gb = gb + graw
        for n in range(NST):
            tscr[2, pl.ds(n * NCH, NCH), :] = ga[n]
        gsum = tscr[2, pl.ds(0, NST, stride=NCH), :]
        for k in range(1, NCH):
            gsum = gsum + tscr[2, pl.ds(k, NST, stride=NCH), :]
        par[c, 0:8, :] = gsum * (a2 * LN2)
        par[c, 8:9, :] = jnp.sum(gb, axis=0, keepdims=True)
        for k in range(NCH):
            rows = pl.ds(k * PITCH, LEN)
            gx_ref[0, pl.ds(k * LEN, LEN), lanes] = gxt[rows, :].astype(BF16)
            gr_ref[0, pl.ds(k * LEN, LEN), lanes] = grt[rows, :].astype(BF16)

    def mixer_state_grads():
        ones = jnp.ones((8, 128), F32)
        for accum, ref in ((gbacc, gin_ref), (gcacc, gout_ref)):
            for n in range(NST):
                rows = [accum[n, pl.ds(k, LEN, stride=NCH), :] for k in range(NCH)]
                full = jnp.concatenate(rows, 0)
                line = lax.dot_general(
                    ones, full, NT, preferred_element_type=F32, precision=lax.Precision.HIGHEST
                )
                gred[n : n + 1, :] = line[0:1, :]
            ref[0] = gred[...].astype(BF16)

    def params_rows():
        @pl.when(s < TILES)
        def _():
            scatter_wait_recv(pgat, c_recv)
            total = pgat[0]
            for i in range(1, NSEQ):
                total = total + pgat[i]
            psm[...] = total
            p4[g] = total

            @pl.loop(0, NGRP)
            def _(i):
                @pl.when(i != g)
                def _():
                    pltpu.make_async_remote_copy(
                        src_ref=psm, dst_ref=p4.at[g], send_sem=d_send, recv_sem=d_recv,
                        device_id={"grp": i}, device_id_type=MESH,
                    ).start()

    def params_groups():
        @pl.when(s < TILES)
        def _():
            head = p4.at[pl.ds(0, NGRP - 1)]
            pltpu.make_async_copy(head, head, d_recv).wait()
            final = (p4[0] + p4[1]) + (p4[2] + p4[3])
            pfin[...] = final
            pout[s] = final
            spread_out(lambda i: pfin, pout, e_send, e_recv)

    def params_store():
        tiles_wait(pout, e_recv)

        @pl.loop(0, TILES)
        def _(c):
            lanes = pl.ds(pl.multiple_of(c * 128, 128), 128)
            gdec_ref[:, lanes] = pout[c, 0:8, :]
            gbias_ref[:, lanes] = pout[c, 8:9, :]
            gskip_ref[:, lanes] = pout[c, 9:10, :]

    def mixer_drain():
        tiles_wait(tot, a_send)
        tiles_wait(dtot, t_send)
        tiles_wait(par, c_send)

        @pl.when(s < TILES)
        def _():
            part = cbuf.at[pl.ds(0, NSEQ - 1)]
            pltpu.make_async_copy(part, part, b_send).wait()
            part = p4.at[pl.ds(0, NGRP - 1)]
            pltpu.make_async_copy(part, part, d_send).wait()
            part = pgat.at[pl.ds(0, NSEQ - 1)]
            pltpu.make_async_copy(part, part, e_send).wait()

    def run_hooks(hooks, i):
        for at, action in hooks:

            @pl.when(i == at)
            def _():
                action()

    def tiles(body, start, stop, hooks):
        @pl.loop(start, stop)
        def _(c):
            run_hooks(hooks, c)
            body(c)

    K, VV, Q, DO = range(4)

    def send(*pairs):
        def go():
            for t, h in pairs:
                send_in(t, h)

        return go

    send((K, 0), (VV, 0))()
    for h in range(HPD):
        forward_own(h)
    mixer_tables()
    for copy in mix_in:
        copy.wait()
    tiles(mixer_local, 0, TILES, [(4, send((Q, 0)))])
    scatter(tot, gath, a_send, a_recv)
    scatter(dtot, gdt, t_send, t_recv)
    send((DO, 0))()
    gbacc[...] = jnp.zeros(gbacc.shape, F32)
    gcacc[...] = jnp.zeros(gcacc.shape, F32)
    mixer_prefix()
    forward_rest(0)
    send((K, 1), (VV, 1), (K, 2), (VV, 2), (Q, 1), (DO, 1), (Q, 2), (DO, 2))()
    tiles_wait(cin, b_recv)
    tiles(mixer_back, 0, TILES // 2, [(9, lambda: forward_rest(1))])
    attention(0, [(2, lambda: forward_rest(2))])
    tiles(mixer_back, TILES // 2, TILES, [])
    scatter(par, pgat, c_send, c_recv)
    mixer_state_grads()
    attention(1, [])
    finish_head(0)
    params_rows()
    attention(2, [])
    params_groups()
    finish_head(1)
    finish_head(2)
    params_store()
    mixer_drain()
    drain()


def store_results(*refs):
    n = len(refs) // 2
    srcs, outs, sems = refs[:n], refs[n : 2 * n], refs[2 * n]
    copies = [pltpu.make_async_copy(a, b, sems.at[i]) for i, (a, b) in enumerate(zip(srcs, outs))]
    for copy in copies:
        copy.start()
    for copy in copies:
        copy.wait()


def per_device(queries, keys, values, cot_attn, x, raw, bin_, cout, cot, decay_log, step_bias, skip_gain):
    vm = pl.BlockSpec(memory_space=pltpu.VMEM)
    hbm = pl.BlockSpec(memory_space=pl.ANY)
    att = jax.ShapeDtypeStruct((1, BLK, 12 * HD), BF16)
    mix = jax.ShapeDtypeStruct((1, TOK, INNER), BF16)
    stt = jax.ShapeDtypeStruct((1, NST, TOK), BF16)
    chan = jax.ShapeDtypeStruct((1, INNER), F32)
    V = pltpu.VMEM
    shapes = (att, att, att, mix, mix, stt, stt, jax.ShapeDtypeStruct((NST, INNER), F32), chan, chan)
    D = pltpu.SemaphoreType.DMA
    scratch = [
        V((HPD, OWN, HD), BF16), V((HPD, OWN, HD), BF16), V((HPD, 2 * OWN, HD), BF16), V((HPD, 2 * OWN, HD), BF16),
        V((HPD, 2, 2 * OWN, HD), F32), V((HPD, OWN, HD), BF16),
        V((HPD, 2, OWN, HD), BF16), V((HPD, 2, OWN, HD), BF16), V((HPD, 2, OWN, HD), BF16),
        *[V((1, TOK, INNER), BF16)] * 3, D((3,)),
        *[V((TILES, NCH * PITCH, 128), F32)] * 4,
        V((TILES, LEN, NST, NCH, 128), F32), V((TILES, NST, 128), F32),
        V((NST, LEN, NCH, 128), F32), V((NST, LEN, NCH, 128), F32), V((NCH * PITCH, 128), F32),
        V((3, NST * NCH, 128), F32),
        *[V((TILES, NCH, NST, 128), F32)] * 4,
        V((TILES, 16, 128), BF16), V((TILES, 1, 128), F32), V((NSEQ, 16, 128), BF16), V((NSEQ, 1, 128), F32),
        V((NSEQ, NST, 128), F32), V((NSEQ, 16, 128), BF16), V((TILES, 16, 128), BF16),
        V((LEN, NST, NCH, 128), F32), V((NCH * PITCH, 128), F32), V((NCH * PITCH, 128), F32),
        V((NST, LEN * NCH, 128), F32), V((NST, LEN * NCH, 128), F32), V((NST, 128), F32),
        V((TILES, 10, 128), F32), V((NSEQ, 10, 128), F32), V((10, 128), F32), V((NGRP, 10, 128), F32),
        V((10, 128), F32), V((TILES, 10, 128), F32),
        D((4, HPD, ROW - 1)), D((4, HPD, ROW - 1)), D((4, HPD)),
        *[D((2, HPD, ROW))] * 4,
        D((3, HPD, ROW)), D((3, HPD, ROW)), D((3, HPD)),
        *[D(())] * 12,
    ]
    res = pl.pallas_call(
        kernel,
        out_shape=tuple(V(a.shape, a.dtype) for a in shapes),
        in_specs=[hbm] * 6 + [vm] * 2 + [hbm] + [vm] * 3,
        out_specs=(vm,) * 10,
        scratch_shapes=scratch,
        compiler_params=pltpu.CompilerParams(
            collective_id=0, has_side_effects=True, vmem_limit_bytes=56 * 1024 * 1024
        ),
    )(queries, keys, values, cot_attn, x, raw, bin_, cout, cot, decay_log, step_bias.reshape(1, -1), skip_gain.reshape(1, -1))
    res = pl.pallas_call(
        store_results,
        out_shape=shapes,
        in_specs=[vm] * len(shapes),
        out_specs=(hbm,) * len(shapes),
        scratch_shapes=[D((len(shapes),))],
        compiler_params=pltpu.CompilerParams(vmem_limit_bytes=4 * 1024 * 1024),
    )(*[pltpu.with_memory_space_constraint(a, pltpu.VMEM) for a in res])
    return tuple(res[:8]) + (res[8].reshape(-1), res[9].reshape(-1))


def solution(mesh):
    tok = P("grp", "seq", None)
    stt = P("grp", None, "seq")
    return jax.shard_map(
        per_device,
        mesh=mesh,
        in_specs=(tok,) * 4 + (tok, tok, stt, stt, tok, P(), P(), P()),
        out_specs=(tok,) * 3 + (tok, tok, stt, stt, P(), P(), P()),
        check_vma=False,
    )
```

```python
import functools

import jax
import jax.numpy as jnp
from jax import lax
from jax.experimental import pallas as pl
from jax.experimental.pallas import tpu as pltpu
from jax.sharding import PartitionSpec as P

MESH = pl.DeviceIdType.MESH
F32 = jnp.float32
BF16 = jnp.bfloat16

NSEQ = 32
NGRP = 4
ROW = 4
NROW = NSEQ // ROW
BLK = 256
OWN = ROW * BLK
HPD = 3
HD = 128
TOK = 128
NCH = 8
LEN = TOK // NCH
PITCH = 24
NST = 8
TILES = 24
INNER = TILES * 128
LOG2E = 1.4426950408889634
LN2 = 0.6931471805599453
NEG = -1e30
SCALE = HD**-0.5

AWAY = (2, 1, 3, 0)

NT = (((1,), (1,)), ((), ()))
NN = (((1,), (0,)), ((), ()))
TN = (((0,), (0,)), ((), ()))


def dot(a, b, dims):
    return lax.dot_general(a, b, dims, preferred_element_type=F32)


def kernel(
    q_hbm, k_hbm, v_hbm, do_hbm, x_hbm, raw_hbm, bin_ref, cout_ref, cot_hbm, dl_ref, bias_ref, skip_ref,
    dq_hbm, dk_hbm, dv_hbm, gx_ref, gr_ref, gin_ref, gout_ref, gdec_ref, gbias_ref, gskip_ref,
    qs, dos, ks, vs, acc, qout, retout, retin, fin,
    x_ref, raw_ref, cot_ref, mix_sem, dts, xs, cts, sgs, avs, a2s, btab, ctab, natt, tscr, pds, pes, sds, sbs, tot, dtot, gath, gdt, ahead, cbuf, cin,
    ahs, gxt, grt, gbacc, gcacc, gred, par, pgat, psm, p4, pfin, pout,
    in_send, in_recv, in_loc, fw_send, fw_recv, rt_send, rt_recv, o_send, o_recv, o_loc,
    a_send, a_recv, t_send, t_recv, b_send, b_recv, c_send, c_recv, d_send, d_recv, e_send, e_recv,
):
    s = lax.axis_index("seq")
    g = lax.axis_index("grp")
    col = lax.rem(s, ROW)
    base = s - col
    row = s // ROW
    first = row == 0
    last = row == NROW - 1

    mix_in = [
        pltpu.make_async_copy(src, dst, mix_sem.at[i])
        for i, (src, dst) in enumerate(((x_hbm, x_ref), (raw_hbm, raw_ref), (cot_hbm, cot_ref)))
    ]
    for copy in mix_in:
        copy.start()

    barrier = pltpu.get_barrier_semaphore()

    @pl.loop(0, NSEQ)
    def _(i):
        @pl.when(i != s)
        def _():
            pl.semaphore_signal(barrier, inc=1, device_id={"seq": i}, device_id_type=MESH)

    @pl.loop(0, NGRP)
    def _(i):
        @pl.when(i != g)
        def _():
            pl.semaphore_signal(barrier, inc=1, device_id={"grp": i}, device_id_type=MESH)

    pl.semaphore_wait(barrier, NSEQ + NGRP - 2)

    srcs = (k_hbm, v_hbm, q_hbm, do_hbm)
    dsts = (ks, vs, qs, dos)
    lead = (OWN, OWN, 0, 0)

    def in_copy(t, h, off):
        peer = lax.rem(col + off, ROW)
        lanes = pl.ds(pl.multiple_of((peer * HPD + h) * HD, HD), HD)
        rows = pl.ds(pl.multiple_of(lead[t] + col * BLK, BLK), BLK)
        return pltpu.make_async_remote_copy(
            src_ref=srcs[t].at[0, :, lanes],
            dst_ref=dsts[t].at[h, rows, :],
            send_sem=in_send.at[t, h, off - 1],
            recv_sem=in_recv.at[t, h, off - 1],
            device_id={"seq": base + peer},
            device_id_type=MESH,
        )

    def in_wait(t, h, off):
        peer = lax.rem(col + ROW - off, ROW)
        lanes = pl.ds(pl.multiple_of((col * HPD + h) * HD, HD), HD)
        rows = pl.ds(pl.multiple_of(lead[t] + peer * BLK, BLK), BLK)
        pltpu.make_async_remote_copy(
            src_ref=srcs[t].at[0, :, lanes],
            dst_ref=dsts[t].at[h, rows, :],
            send_sem=in_send.at[t, h, off - 1],
            recv_sem=in_recv.at[t, h, off - 1],
            device_id={"seq": base + peer},
            device_id_type=MESH,
        ).wait_recv()

    def in_local(t, h):
        lanes = pl.ds(pl.multiple_of((col * HPD + h) * HD, HD), HD)
        rows = pl.ds(pl.multiple_of(lead[t] + col * BLK, BLK), BLK)
        return pltpu.make_async_copy(
            srcs[t].at[0, :, lanes], dsts[t].at[h, rows, :], in_loc.at[t, h]
        )

    def send_in(t, h):
        for off in range(1, ROW):
            in_copy(t, h, off).start()
        in_local(t, h).start()

    def block_rows(start, j):
        return pl.ds(pl.multiple_of(start + j * BLK, BLK), BLK)

    def fw_copy(t, h, j, own=False):
        lanes = pl.ds(pl.multiple_of((col * HPD + h) * HD, HD), HD)
        return pltpu.make_async_remote_copy(
            src_ref=srcs[t].at[0, :, lanes] if own else dsts[t].at[h, block_rows(OWN, j), :],
            dst_ref=dsts[t].at[h, block_rows(0, j), :],
            send_sem=fw_send.at[t, h, j],
            recv_sem=fw_recv.at[t, h, j],
            device_id={"seq": lax.rem(s + ROW, NSEQ)},
            device_id_type=MESH,
        )

    def forward_own(h):
        @pl.when(jnp.logical_not(last))
        def _():
            for t in range(2):
                fw_copy(t, h, col, own=True).start()

    def forward_rest(h):
        for off in range(1, ROW):
            for t in range(2):
                in_wait(t, h, off)

            @pl.when(jnp.logical_not(last))
            def _():
                for t in range(2):
                    fw_copy(t, h, lax.rem(col + ROW - off, ROW)).start()

    def rt_copy(t, h, j):
        return pltpu.make_async_remote_copy(
            src_ref=retout.at[h, t, block_rows(0, j), :],
            dst_ref=retin.at[h, t, block_rows(0, j), :],
            send_sem=rt_send.at[t, h, j],
            recv_sem=rt_recv.at[t, h, j],
            device_id={"seq": lax.rem(s + NSEQ - ROW, NSEQ)},
            device_id_type=MESH,
        )

    outs = (dk_hbm, dv_hbm, dq_hbm)

    def out_src(t, h):
        return qout.at[h] if t == 2 else fin.at[h, t]

    def out_remote(t, h, j):
        lanes = pl.ds(pl.multiple_of((col * HPD + h) * HD, HD), HD)
        return pltpu.make_async_remote_copy(
            src_ref=out_src(t, h).at[block_rows(0, j), :],
            dst_ref=outs[t].at[0, :, lanes],
            send_sem=o_send.at[t, h, j],
            recv_sem=o_recv.at[t, h, col],
            device_id={"seq": base + j},
            device_id_type=MESH,
        )

    def out_local(t, h):
        lanes = pl.ds(pl.multiple_of((col * HPD + h) * HD, HD), HD)
        return pltpu.make_async_copy(
            out_src(t, h).at[block_rows(0, col), :], outs[t].at[0, :, lanes], o_loc.at[t, h]
        )

    def out_wait(t, h, peer):
        lanes = pl.ds(pl.multiple_of((peer * HPD + h) * HD, HD), HD)
        pltpu.make_async_remote_copy(
            src_ref=out_src(t, h).at[block_rows(0, col), :],
            dst_ref=outs[t].at[0, :, lanes],
            send_sem=o_send.at[t, h, peer],
            recv_sem=o_recv.at[t, h, peer],
            device_id={"seq": base + peer},
            device_id_type=MESH,
        ).wait_recv()

    def out_start(ts, h, j):
        @pl.when(j == col)
        def _():
            for t in ts:
                out_local(t, h).start()

        @pl.when(j != col)
        def _():
            for t in ts:
                out_remote(t, h, j).start()

    def attention(h, hooks, at_once=True):
        for t in range(4):
            in_local(t, h).wait()
        for t in range(2, 4):
            for off in range(1, ROW):
                in_wait(t, h, off)

        @pl.when(jnp.logical_not(first))
        def _():
            for j in range(ROW):
                for t in range(2):
                    fw_copy(t, h, j).wait_recv()

        @pl.when(first)
        def _():
            zeros = jnp.zeros((OWN, HD), BF16)
            ks[h, pl.ds(0, OWN), :] = zeros
            vs[h, pl.ds(0, OWN), :] = zeros

        acc[h] = jnp.zeros(acc.shape[1:], F32)
        key_pos = lax.broadcasted_iota(jnp.int32, (BLK, BLK), 0)
        qry_pos = lax.broadcasted_iota(jnp.int32, (BLK, BLK), 1)
        causal = key_pos <= qry_pos

        @pl.loop(0, ROW)
        def _(i):
            run_hooks(hooks, i)
            at = pl.multiple_of(i * BLK, BLK)
            qrows = pl.ds(at, BLK)
            krows = pl.ds(at, OWN + BLK)
            qb = qs[h, qrows, :]
            dob = dos[h, qrows, :]
            kb = ks[h, krows, :]
            vb = vs[h, krows, :]
            st = dot(kb, qb, NT)
            dpt = dot(vb, dob, NT)

            def bias(kt):
                return jnp.where(jnp.logical_and(first, i + kt < ROW), NEG, 0.0).astype(F32)

            parts = [jnp.where(causal, st[OWN:], st[:BLK] + bias(0))]
            for kt in range(1, ROW):
                parts.append(st[kt * BLK : (kt + 1) * BLK] + bias(kt))
            scores = jnp.concatenate(parts, 0)
            dp = jnp.concatenate([jnp.where(causal, dpt[OWN:], dpt[:BLK]), dpt[BLK:OWN]], 0)
            top = jnp.max(scores, axis=0, keepdims=True)
            raw = jnp.exp2((scores - top) * (SCALE * LOG2E))
            prob = raw * (1.0 / jnp.sum(raw, axis=0, keepdims=True))
            pb = prob.astype(BF16)
            delta = jnp.sum(pb.astype(F32) * dp, axis=0, keepdims=True)
            ds = prob * (dp - delta)
            zero = jnp.zeros((BLK, BLK), F32)
            pfull = jnp.concatenate(
                [jnp.where(causal, zero, prob[:BLK]).astype(BF16), pb[BLK:], jnp.where(causal, prob[:BLK], zero).astype(BF16)], 0
            )
            dsb = ds.astype(BF16)
            dfull = jnp.concatenate(
                [jnp.where(causal, zero, ds[:BLK]).astype(BF16), dsb[BLK:], jnp.where(causal, ds[:BLK], zero).astype(BF16)], 0
            )
            acc[h, 1, krows, :] += dot(pfull, dob, NN)
            acc[h, 0, krows, :] += dot(dfull, qb, NN)
            dq = dot(kb, dfull, TN)
            qout[h, qrows, :] = (dq.T * SCALE).astype(BF16)

            out_start((2,), h, i)

            @pl.when(jnp.logical_not(first))
            def _():
                retout[h, 0, qrows, :] = (acc[h, 0, qrows, :] * SCALE).astype(BF16)
                retout[h, 1, qrows, :] = acc[h, 1, qrows, :].astype(BF16)
                if at_once:
                    for t in range(2):
                        rt_copy(t, h, i).start()

        if not at_once:

            @pl.when(jnp.logical_not(first))
            def _():
                for off in AWAY:
                    for t in range(2):
                        rt_copy(t, h, lax.rem(col + off, ROW)).start()

    def finish_head(h):
        for off in AWAY:
            j = lax.rem(col + off, ROW)
            rows = block_rows(0, j)
            own = block_rows(OWN, j)
            for t in range(2):
                scale = SCALE if t == 0 else 1.0

                @pl.when(last)
                def _():
                    fin[h, t, rows, :] = (acc[h, t, own, :] * scale).astype(BF16)

                @pl.when(jnp.logical_not(last))
                def _():
                    rt_copy(t, h, j).wait_recv()
                    mine = acc[h, t, own, :] * scale
                    fin[h, t, rows, :] = (mine + retin[h, t, rows, :].astype(F32)).astype(BF16)

            out_start((0, 1), h, j)

    def drain():
        @pl.loop(0, HPD)
        def _(h):
            for t in range(4):
                for off in range(1, ROW):
                    in_copy(t, h, off).wait_send()

            @pl.loop(0, ROW)
            def _(j):
                for t in range(2):

                    @pl.when(jnp.logical_not(last))
                    def _():
                        fw_copy(t, h, j).wait_send()

                    @pl.when(jnp.logical_not(first))
                    def _():
                        rt_copy(t, h, j).wait_send()

                @pl.when(j == col)
                def _():
                    for t in range(3):
                        out_local(t, h).wait()

                @pl.when(j != col)
                def _():
                    for t in range(3):
                        out_remote(t, h, j).wait_send()
                        out_wait(t, h, j)

    def mixer_tables():
        bin32 = bin_ref[0].astype(F32)
        cout32 = cout_ref[0].astype(F32)
        for tab, rows32 in ((btab, bin32), (ctab, cout32)):
            for n in range(NST):
                wide = jnp.broadcast_to(rows32[n : n + 1, :], (TOK, TOK)).T
                for k in range(NCH):
                    natt[pl.ds(k * PITCH, LEN), :] = wide[k * LEN : (k + 1) * LEN]
                for j in range(LEN):
                    tab[n, j] = natt[pl.ds(j, NCH, stride=PITCH), :]

    def spread(block, n):
        return jnp.broadcast_to(block[n : n + 1, :], (NCH, 128))

    def mixer_local(c):
        lanes = pl.ds(pl.multiple_of(c * 128, 128), 128)
        x = x_ref[0, :, lanes].astype(F32)
        z = raw_ref[0, :, lanes].astype(F32) + bias_ref[:, lanes]
        ct = cot_ref[0, :, lanes].astype(F32)
        small = jnp.exp(-jnp.abs(z))
        dt = jnp.maximum(z, 0.0) + jnp.log1p(small)
        sg = jnp.where(z >= 0.0, 1.0, small) / (1.0 + small)
        par[c, 9:10, :] = jnp.sum(ct * x, axis=0, keepdims=True)
        for k in range(NCH):
            rows = pl.ds(k * PITCH, LEN)
            part = slice(k * LEN, (k + 1) * LEN)
            dts[c, rows, :] = dt[part]
            xs[c, rows, :] = x[part]
            cts[c, rows, :] = ct[part]
            sgs[c, rows, :] = sg[part]
        a2 = -jnp.exp(dl_ref[:, lanes]) * LOG2E
        a2s[c] = a2
        rate = [spread(a2, n) for n in range(NST)]
        state = [jnp.zeros((NCH, 128), F32) for _ in range(NST)]
        decay = [jnp.ones((NCH, 128), F32) for _ in range(NST)]
        back = [jnp.zeros((NCH, 128), F32) for _ in range(NST)]
        for j in range(LEN):
            rows = pl.ds(j, NCH, stride=PITCH)
            dtj = dts[c, rows, :]
            uj = dtj * xs[c, rows, :]
            cj = cts[c, rows, :]
            for n in range(NST):
                a = jnp.exp2(dtj * rate[n])
                avs[c, j, n] = a
                state[n] = a * state[n] + uj * btab[n, j]
                decay[n] = a * decay[n]
                back[n] = back[n] + decay[n] * (cj * ctab[n, j])
        for n in range(NST):
            rows = pl.ds(n * NCH, NCH)
            tscr[0, rows, :] = state[n]
            tscr[1, rows, :] = decay[n]
            tscr[2, rows, :] = back[n]
        ek = [tscr[0, pl.ds(k, NST, stride=NCH), :] for k in range(NCH)]
        dk = [tscr[1, pl.ds(k, NST, stride=NCH), :] for k in range(NCH)]
        bk = [tscr[2, pl.ds(k, NST, stride=NCH), :] for k in range(NCH)]
        pd = jnp.ones((NST, 128), F32)
        pe = jnp.zeros((NST, 128), F32)
        for k in range(NCH):
            pds[c, k] = pd
            pes[c, k] = pe
            pe = dk[k] * pe + ek[k]
            pd = dk[k] * pd
        sd = jnp.ones((NST, 128), F32)
        sb = jnp.zeros((NST, 128), F32)
        for k in reversed(range(NCH)):
            sds[c, k] = sd
            sbs[c, k] = sb
            sb = dk[k] * sb + bk[k]
            sd = dk[k] * sd
        tot[c] = jnp.concatenate([pe, sb], 0).astype(BF16)
        dtot[c] = jnp.sum(dt, axis=0, keepdims=True)

    def scatter(src, dst, send, recv):
        @pl.loop(0, TILES)
        def _(j):
            @pl.when(j != s)
            def _():
                pltpu.make_async_remote_copy(
                    src_ref=src.at[j], dst_ref=dst.at[s], send_sem=send, recv_sem=recv,
                    device_id={"seq": j}, device_id_type=MESH,
                ).start()

        @pl.when(s < TILES)
        def _():
            dst[s] = src[s]

    def scatter_wait_recv(dst, sem):
        head = dst.at[pl.ds(0, NSEQ - 1)]
        pltpu.make_async_copy(head, head, sem).wait()

    def tiles_wait(ref, sem):
        @pl.when(s < TILES)
        def _():
            part = ref.at[pl.ds(0, TILES - 1)]
            pltpu.make_async_copy(part, part, sem).wait()

        @pl.when(s >= TILES)
        def _():
            part = ref.at[pl.ds(0, TILES)]
            pltpu.make_async_copy(part, part, sem).wait()

    def spread_out(src_of, dst, send, recv):
        @pl.loop(0, NSEQ)
        def _(i):
            @pl.when(i != s)
            def _():
                pltpu.make_async_remote_copy(
                    src_ref=src_of(i), dst_ref=dst.at[s], send_sem=send, recv_sem=recv,
                    device_id={"seq": i}, device_id_type=MESH,
                ).start()

    def mixer_prefix():
        @pl.when(s < TILES)
        def _():
            scatter_wait_recv(gath, a_recv)
            scatter_wait_recv(gdt, t_recv)
            a2 = a2s[s]
            carry = jnp.zeros((NST, 128), F32)
            for i in range(NSEQ):
                ahead[i] = carry
                carry = jnp.exp2(a2 * gdt[i]) * carry + gath[i].astype(F32)[0:8]
            carry = jnp.zeros((NST, 128), F32)
            for i in reversed(range(NSEQ)):
                cbuf[i] = jnp.concatenate([ahead[i], carry], 0).astype(BF16)
                carry = jnp.exp2(a2 * gdt[i]) * carry + gath[i].astype(F32)[8:16]
            spread_out(lambda i: cbuf.at[i], cin, b_send, b_recv)
            cin[s] = cbuf[s]

    def mixer_back(c):
        lanes = pl.ds(pl.multiple_of(c * 128, 128), 128)
        entering = cin[c].astype(F32)
        hin = entering[0:8]
        gin = entering[8:16]
        for k in range(NCH):
            rows = pl.ds(k * NST, NST)
            tscr[0, rows, :] = pds[c, k] * hin + pes[c, k]
            tscr[1, rows, :] = sds[c, k] * gin + sbs[c, k]
        state = [tscr[0, pl.ds(n, NCH, stride=NST), :] for n in range(NST)]
        a2 = a2s[c]
        for j in range(LEN):
            rows = pl.ds(j, NCH, stride=PITCH)
            uj = dts[c, rows, :] * xs[c, rows, :]
            cj = cts[c, rows, :]
            for n in range(NST):
                ah = avs[c, j, n] * state[n]
                ahs[j, n] = ah
                state[n] = ah + uj * btab[n, j]
                gcacc[n, pl.ds(j * NCH, NCH), :] += cj * state[n]
        adj = [tscr[1, pl.ds(n, NCH, stride=NST), :] for n in range(NST)]
        ga = [jnp.zeros((NCH, 128), F32) for _ in range(NST)]
        rate = [spread(a2, n) for n in range(NST)]
        skip = jnp.broadcast_to(skip_ref[:, lanes], (NCH, 128))
        gb = jnp.zeros((NCH, 128), F32)
        for j in reversed(range(LEN)):
            rows = pl.ds(j, NCH, stride=PITCH)
            dtj = dts[c, rows, :]
            xj = xs[c, rows, :]
            uj = dtj * xj
            cj = cts[c, rows, :]
            proj = None
            gdt = None
            for n in range(NST):
                gn = adj[n] + ctab[n, j] * cj
                gbacc[n, pl.ds(j * NCH, NCH), :] += gn * uj
                w = gn * ahs[j, n]
                ga[n] = ga[n] + w * dtj
                p1 = gn * btab[n, j]
                p2 = w * rate[n]
                proj = p1 if proj is None else proj + p1
                gdt = p2 if gdt is None else gdt + p2
                adj[n] = avs[c, j, n] * gn
            gxt[rows, :] = skip * cj + dtj * proj
            graw = (xj * proj + gdt * LN2) * sgs[c, rows, :]
            grt[rows, :] = graw
            gb = gb + graw
        for n in range(NST):
            tscr[2, pl.ds(n * NCH, NCH), :] = ga[n]
        gsum = tscr[2, pl.ds(0, NST, stride=NCH), :]
        for k in range(1, NCH):
            gsum = gsum + tscr[2, pl.ds(k, NST, stride=NCH), :]
        par[c, 0:8, :] = gsum * (a2 * LN2)
        par[c, 8:9, :] = jnp.sum(gb, axis=0, keepdims=True)
        for k in range(NCH):
            rows = pl.ds(k * PITCH, LEN)
            gx_ref[0, pl.ds(k * LEN, LEN), lanes] = gxt[rows, :].astype(BF16)
            gr_ref[0, pl.ds(k * LEN, LEN), lanes] = grt[rows, :].astype(BF16)

    def mixer_state_grads():
        ones = jnp.ones((8, 128), F32)
        for accum, ref in ((gbacc, gin_ref), (gcacc, gout_ref)):
            for n in range(NST):
                rows = [accum[n, pl.ds(k, LEN, stride=NCH), :] for k in range(NCH)]
                full = jnp.concatenate(rows, 0)
                line = lax.dot_general(
                    ones, full, NT, preferred_element_type=F32, precision=lax.Precision.HIGHEST
                )
                gred[n : n + 1, :] = line[0:1, :]
            ref[0] = gred[...].astype(BF16)

    def params_rows():
        @pl.when(s < TILES)
        def _():
            scatter_wait_recv(pgat, c_recv)
            total = pgat[0]
            for i in range(1, NSEQ):
                total = total + pgat[i]
            psm[...] = total
            p4[g] = total

            @pl.loop(0, NGRP)
            def _(i):
                @pl.when(i != g)
                def _():
                    pltpu.make_async_remote_copy(
                        src_ref=psm, dst_ref=p4.at[g], send_sem=d_send, recv_sem=d_recv,
                        device_id={"grp": i}, device_id_type=MESH,
                    ).start()

    def params_groups():
        @pl.when(s < TILES)
        def _():
            head = p4.at[pl.ds(0, NGRP - 1)]
            pltpu.make_async_copy(head, head, d_recv).wait()
            final = (p4[0] + p4[1]) + (p4[2] + p4[3])
            pfin[...] = final
            pout[s] = final
            spread_out(lambda i: pfin, pout, e_send, e_recv)

    def params_store():
        tiles_wait(pout, e_recv)

        @pl.loop(0, TILES)
        def _(c):
            lanes = pl.ds(pl.multiple_of(c * 128, 128), 128)
            gdec_ref[:, lanes] = pout[c, 0:8, :]
            gbias_ref[:, lanes] = pout[c, 8:9, :]
            gskip_ref[:, lanes] = pout[c, 9:10, :]

    def mixer_drain():
        tiles_wait(tot, a_send)
        tiles_wait(dtot, t_send)
        tiles_wait(par, c_send)

        @pl.when(s < TILES)
        def _():
            part = cbuf.at[pl.ds(0, NSEQ - 1)]
            pltpu.make_async_copy(part, part, b_send).wait()
            part = p4.at[pl.ds(0, NGRP - 1)]
            pltpu.make_async_copy(part, part, d_send).wait()
            part = pgat.at[pl.ds(0, NSEQ - 1)]
            pltpu.make_async_copy(part, part, e_send).wait()

    def run_hooks(hooks, i):
        for at, action in hooks:

            @pl.when(i == at)
            def _():
                action()

    def tiles(body, start, stop, hooks):
        @pl.loop(start, stop)
        def _(c):
            run_hooks(hooks, c)
            body(c)

    K, VV, Q, DO = range(4)

    def send(*pairs):
        def go():
            for t, h in pairs:
                send_in(t, h)

        return go

    send((K, 0), (VV, 0))()
    for h in range(HPD):
        forward_own(h)
    mixer_tables()
    for copy in mix_in:
        copy.wait()
    tiles(mixer_local, 0, TILES, [(4, send((Q, 0)))])
    scatter(tot, gath, a_send, a_recv)
    scatter(dtot, gdt, t_send, t_recv)
    send((DO, 0))()
    gbacc[...] = jnp.zeros(gbacc.shape, F32)
    gcacc[...] = jnp.zeros(gcacc.shape, F32)
    mixer_prefix()
    forward_rest(0)
    send((K, 1), (VV, 1), (K, 2), (VV, 2), (Q, 1), (DO, 1), (Q, 2), (DO, 2))()
    tiles_wait(cin, b_recv)
    tiles(mixer_back, 0, TILES // 2, [(9, lambda: forward_rest(1))])
    attention(0, [(2, lambda: forward_rest(2))])
    tiles(mixer_back, TILES // 2, TILES, [])
    scatter(par, pgat, c_send, c_recv)
    mixer_state_grads()
    attention(1, [])
    finish_head(0)
    params_rows()
    attention(2, [], at_once=False)
    finish_head(1)
    params_groups()
    finish_head(2)
    params_store()
    mixer_drain()
    drain()


def store_results(*refs):
    n = len(refs) // 2
    srcs, outs, sems = refs[:n], refs[n : 2 * n], refs[2 * n]
    copies = [pltpu.make_async_copy(a, b, sems.at[i]) for i, (a, b) in enumerate(zip(srcs, outs))]
    for copy in copies:
        copy.start()
    for copy in copies:
        copy.wait()


def per_device(queries, keys, values, cot_attn, x, raw, bin_, cout, cot, decay_log, step_bias, skip_gain):
    vm = pl.BlockSpec(memory_space=pltpu.VMEM)
    hbm = pl.BlockSpec(memory_space=pl.ANY)
    att = jax.ShapeDtypeStruct((1, BLK, 12 * HD), BF16)
    mix = jax.ShapeDtypeStruct((1, TOK, INNER), BF16)
    stt = jax.ShapeDtypeStruct((1, NST, TOK), BF16)
    chan = jax.ShapeDtypeStruct((1, INNER), F32)
    V = pltpu.VMEM
    shapes = (att, att, att, mix, mix, stt, stt, jax.ShapeDtypeStruct((NST, INNER), F32), chan, chan)
    D = pltpu.SemaphoreType.DMA
    scratch = [
        V((HPD, OWN, HD), BF16), V((HPD, OWN, HD), BF16), V((HPD, 2 * OWN, HD), BF16), V((HPD, 2 * OWN, HD), BF16),
        V((HPD, 2, 2 * OWN, HD), F32), V((HPD, OWN, HD), BF16),
        V((HPD, 2, OWN, HD), BF16), V((HPD, 2, OWN, HD), BF16), V((HPD, 2, OWN, HD), BF16),
        *[V((1, TOK, INNER), BF16)] * 3, D((3,)),
        *[V((TILES, NCH * PITCH, 128), F32)] * 4,
        V((TILES, LEN, NST, NCH, 128), F32), V((TILES, NST, 128), F32),
        V((NST, LEN, NCH, 128), F32), V((NST, LEN, NCH, 128), F32), V((NCH * PITCH, 128), F32),
        V((3, NST * NCH, 128), F32),
        *[V((TILES, NCH, NST, 128), F32)] * 4,
        V((TILES, 16, 128), BF16), V((TILES, 1, 128), F32), V((NSEQ, 16, 128), BF16), V((NSEQ, 1, 128), F32),
        V((NSEQ, NST, 128), F32), V((NSEQ, 16, 128), BF16), V((TILES, 16, 128), BF16),
        V((LEN, NST, NCH, 128), F32), V((NCH * PITCH, 128), F32), V((NCH * PITCH, 128), F32),
        V((NST, LEN * NCH, 128), F32), V((NST, LEN * NCH, 128), F32), V((NST, 128), F32),
        V((TILES, 10, 128), F32), V((NSEQ, 10, 128), F32), V((10, 128), F32), V((NGRP, 10, 128), F32),
        V((10, 128), F32), V((TILES, 10, 128), F32),
        D((4, HPD, ROW - 1)), D((4, HPD, ROW - 1)), D((4, HPD)),
        *[D((2, HPD, ROW))] * 4,
        D((3, HPD, ROW)), D((3, HPD, ROW)), D((3, HPD)),
        *[D(())] * 12,
    ]
    res = pl.pallas_call(
        kernel,
        out_shape=tuple(V(a.shape, a.dtype) for a in shapes),
        in_specs=[hbm] * 6 + [vm] * 2 + [hbm] + [vm] * 3,
        out_specs=(vm,) * 10,
        scratch_shapes=scratch,
        compiler_params=pltpu.CompilerParams(
            collective_id=0, has_side_effects=True, vmem_limit_bytes=56 * 1024 * 1024
        ),
    )(queries, keys, values, cot_attn, x, raw, bin_, cout, cot, decay_log, step_bias.reshape(1, -1), skip_gain.reshape(1, -1))
    res = pl.pallas_call(
        store_results,
        out_shape=shapes,
        in_specs=[vm] * len(shapes),
        out_specs=(hbm,) * len(shapes),
        scratch_shapes=[D((len(shapes),))],
        compiler_params=pltpu.CompilerParams(vmem_limit_bytes=4 * 1024 * 1024),
    )(*[pltpu.with_memory_space_constraint(a, pltpu.VMEM) for a in res])
    return tuple(res[:8]) + (res[8].reshape(-1), res[9].reshape(-1))


def solution(mesh):
    tok = P("grp", "seq", None)
    stt = P("grp", None, "seq")
    return jax.shard_map(
        per_device,
        mesh=mesh,
        in_specs=(tok,) * 4 + (tok, tok, stt, stt, tok, P(), P(), P()),
        out_specs=(tok,) * 3 + (tok, tok, stt, stt, P(), P(), P()),
        check_vma=False,
    )
```

```python
import functools

import jax
import jax.numpy as jnp
from jax import lax
from jax.experimental import pallas as pl
from jax.experimental.pallas import tpu as pltpu
from jax.sharding import PartitionSpec as P

MESH = pl.DeviceIdType.MESH
F32 = jnp.float32
BF16 = jnp.bfloat16

NSEQ = 32
NGRP = 4
ROW = 4
NROW = NSEQ // ROW
BLK = 256
OWN = ROW * BLK
HPD = 3
HD = 128
TOK = 128
NCH = 8
LEN = TOK // NCH
PITCH = 24
NST = 8
TILES = 24
INNER = TILES * 128
LOG2E = 1.4426950408889634
LN2 = 0.6931471805599453
NEG = -1e30
SCALE = HD**-0.5

AWAY = (2, 1, 3, 0)

NT = (((1,), (1,)), ((), ()))
NN = (((1,), (0,)), ((), ()))
TN = (((0,), (0,)), ((), ()))


def dot(a, b, dims):
    return lax.dot_general(a, b, dims, preferred_element_type=F32)


def kernel(
    q_hbm, k_hbm, v_hbm, do_hbm, x_hbm, raw_hbm, bin_hbm, cout_hbm, cot_hbm, dl_hbm, bias_hbm, skip_hbm,
    dq_hbm, dk_hbm, dv_hbm, gx_ref, gr_ref, gin_ref, gout_ref, gdec_ref, gbias_ref, gskip_ref,
    qs, dos, ks, vs, acc, qout, retout, retin, fin,
    x_ref, raw_ref, cot_ref, bin_ref, cout_ref, dl_ref, bias_ref, skip_ref, mix_sem, dts, xs, cts, sgs, avs, a2s, btab, ctab, natt, tscr, pds, pes, sds, sbs, tot, dtot, gath, gdt, ahead, cbuf, cin,
    ahs, gxt, grt, gbacc, gcacc, gred, par, pgat, psm, p4, pfin, pout,
    heard, in_send, in_recv, in_loc, fw_send, fw_recv, rt_send, rt_recv, o_send, o_recv, o_loc,
    a_send, a_recv, t_send, t_recv, b_send, b_recv, c_send, c_recv, d_send, d_recv, e_send, e_recv,
):
    s = lax.axis_index("seq")
    g = lax.axis_index("grp")
    col = lax.rem(s, ROW)
    base = s - col
    row = s // ROW
    first = row == 0
    last = row == NROW - 1

    mix_in = [
        pltpu.make_async_copy(src, dst, mix_sem.at[i])
        for i, (src, dst) in enumerate(
            (
                (bin_hbm, bin_ref), (cout_hbm, cout_ref), (x_hbm, x_ref), (raw_hbm, raw_ref),
                (cot_hbm, cot_ref), (dl_hbm, dl_ref), (bias_hbm, bias_ref), (skip_hbm, skip_ref),
            )
        )
    ]
    for copy in mix_in:
        copy.start()

    def shifted_row(by):
        return {"seq": lax.rem(s + (by % NROW) * ROW, NSEQ)}

    barrier = pltpu.get_barrier_semaphore()
    for off in range(1, ROW):
        pl.semaphore_signal(barrier, inc=1, device_id={"seq": base + lax.rem(col + off, ROW)}, device_id_type=MESH)
    for by in (1, -1):
        pl.semaphore_signal(barrier, inc=1, device_id=shifted_row(by), device_id_type=MESH)
    for off in range(1, NGRP):
        pl.semaphore_signal(barrier, inc=1, device_id={"grp": lax.rem(g + off, NGRP)}, device_id_type=MESH)
    pl.semaphore_wait(barrier, ROW + NGRP)

    def tell_rows(step):
        for by in ((1, -1), (2, -2), (4,))[step]:
            pl.semaphore_signal(heard.at[step], inc=1, device_id=shifted_row(by), device_id_type=MESH)

    def hear_rows(step):
        pl.semaphore_wait(heard.at[step], (2, 2, 1)[step])

    tell_rows(0)

    srcs = (k_hbm, v_hbm, q_hbm, do_hbm)
    dsts = (ks, vs, qs, dos)
    lead = (OWN, OWN, 0, 0)

    def in_copy(t, h, off):
        peer = lax.rem(col + off, ROW)
        lanes = pl.ds(pl.multiple_of((peer * HPD + h) * HD, HD), HD)
        rows = pl.ds(pl.multiple_of(lead[t] + col * BLK, BLK), BLK)
        return pltpu.make_async_remote_copy(
            src_ref=srcs[t].at[0, :, lanes],
            dst_ref=dsts[t].at[h, rows, :],
            send_sem=in_send.at[t, h, off - 1],
            recv_sem=in_recv.at[t, h, off - 1],
            device_id={"seq": base + peer},
            device_id_type=MESH,
        )

    def in_wait(t, h, off):
        peer = lax.rem(col + ROW - off, ROW)
        lanes = pl.ds(pl.multiple_of((col * HPD + h) * HD, HD), HD)
        rows = pl.ds(pl.multiple_of(lead[t] + peer * BLK, BLK), BLK)
        pltpu.make_async_remote_copy(
            src_ref=srcs[t].at[0, :, lanes],
            dst_ref=dsts[t].at[h, rows, :],
            send_sem=in_send.at[t, h, off - 1],
            recv_sem=in_recv.at[t, h, off - 1],
            device_id={"seq": base + peer},
            device_id_type=MESH,
        ).wait_recv()

    def in_local(t, h):
        lanes = pl.ds(pl.multiple_of((col * HPD + h) * HD, HD), HD)
        rows = pl.ds(pl.multiple_of(lead[t] + col * BLK, BLK), BLK)
        return pltpu.make_async_copy(
            srcs[t].at[0, :, lanes], dsts[t].at[h, rows, :], in_loc.at[t, h]
        )

    def send_in(t, h):
        for off in range(1, ROW):
            in_copy(t, h, off).start()
        in_local(t, h).start()

    def block_rows(start, j):
        return pl.ds(pl.multiple_of(start + j * BLK, BLK), BLK)

    def fw_copy(t, h, j, own=False):
        lanes = pl.ds(pl.multiple_of((col * HPD + h) * HD, HD), HD)
        return pltpu.make_async_remote_copy(
            src_ref=srcs[t].at[0, :, lanes] if own else dsts[t].at[h, block_rows(OWN, j), :],
            dst_ref=dsts[t].at[h, block_rows(0, j), :],
            send_sem=fw_send.at[t, h, j],
            recv_sem=fw_recv.at[t, h, j],
            device_id={"seq": lax.rem(s + ROW, NSEQ)},
            device_id_type=MESH,
        )

    def forward_own(h):
        @pl.when(jnp.logical_not(last))
        def _():
            for t in range(2):
                fw_copy(t, h, col, own=True).start()

    def forward_rest(h):
        for off in range(1, ROW):
            for t in range(2):
                in_wait(t, h, off)

            @pl.when(jnp.logical_not(last))
            def _():
                for t in range(2):
                    fw_copy(t, h, lax.rem(col + ROW - off, ROW)).start()

    def rt_copy(t, h, j):
        return pltpu.make_async_remote_copy(
            src_ref=retout.at[h, t, block_rows(0, j), :],
            dst_ref=retin.at[h, t, block_rows(0, j), :],
            send_sem=rt_send.at[t, h, j],
            recv_sem=rt_recv.at[t, h, j],
            device_id={"seq": lax.rem(s + NSEQ - ROW, NSEQ)},
            device_id_type=MESH,
        )

    outs = (dk_hbm, dv_hbm, dq_hbm)

    def out_src(t, h):
        return qout.at[h] if t == 2 else fin.at[h, t]

    def out_remote(t, h, j):
        lanes = pl.ds(pl.multiple_of((col * HPD + h) * HD, HD), HD)
        return pltpu.make_async_remote_copy(
            src_ref=out_src(t, h).at[block_rows(0, j), :],
            dst_ref=outs[t].at[0, :, lanes],
            send_sem=o_send.at[t, h, j],
            recv_sem=o_recv.at[t, h, col],
            device_id={"seq": base + j},
            device_id_type=MESH,
        )

    def out_local(t, h):
        lanes = pl.ds(pl.multiple_of((col * HPD + h) * HD, HD), HD)
        return pltpu.make_async_copy(
            out_src(t, h).at[block_rows(0, col), :], outs[t].at[0, :, lanes], o_loc.at[t, h]
        )

    def out_wait(t, h, peer):
        lanes = pl.ds(pl.multiple_of((peer * HPD + h) * HD, HD), HD)
        pltpu.make_async_remote_copy(
            src_ref=out_src(t, h).at[block_rows(0, col), :],
            dst_ref=outs[t].at[0, :, lanes],
            send_sem=o_send.at[t, h, peer],
            recv_sem=o_recv.at[t, h, peer],
            device_id={"seq": base + peer},
            device_id_type=MESH,
        ).wait_recv()

    def out_start(ts, h, j):
        @pl.when(j == col)
        def _():
            for t in ts:
                out_local(t, h).start()

        @pl.when(j != col)
        def _():
            for t in ts:
                out_remote(t, h, j).start()

    def attention(h, hooks, at_once=True):
        for t in range(4):
            in_local(t, h).wait()
        for t in range(2, 4):
            for off in range(1, ROW):
                in_wait(t, h, off)

        @pl.when(jnp.logical_not(first))
        def _():
            for j in range(ROW):
                for t in range(2):
                    fw_copy(t, h, j).wait_recv()

        @pl.when(first)
        def _():
            zeros = jnp.zeros((OWN, HD), BF16)
            ks[h, pl.ds(0, OWN), :] = zeros
            vs[h, pl.ds(0, OWN), :] = zeros

        acc[h] = jnp.zeros(acc.shape[1:], F32)
        key_pos = lax.broadcasted_iota(jnp.int32, (BLK, BLK), 0)
        qry_pos = lax.broadcasted_iota(jnp.int32, (BLK, BLK), 1)
        causal = key_pos <= qry_pos

        @pl.loop(0, ROW)
        def _(i):
            run_hooks(hooks, i)
            at = pl.multiple_of(i * BLK, BLK)
            qrows = pl.ds(at, BLK)
            krows = pl.ds(at, OWN + BLK)
            qb = qs[h, qrows, :]
            dob = dos[h, qrows, :]
            kb = ks[h, krows, :]
            vb = vs[h, krows, :]
            st = dot(kb, qb, NT)
            dpt = dot(vb, dob, NT)

            def bias(kt):
                return jnp.where(jnp.logical_and(first, i + kt < ROW), NEG, 0.0).astype(F32)

            parts = [jnp.where(causal, st[OWN:], st[:BLK] + bias(0))]
            for kt in range(1, ROW):
                parts.append(st[kt * BLK : (kt + 1) * BLK] + bias(kt))
            scores = jnp.concatenate(parts, 0)
            dp = jnp.concatenate([jnp.where(causal, dpt[OWN:], dpt[:BLK]), dpt[BLK:OWN]], 0)
            top = jnp.max(scores, axis=0, keepdims=True)
            raw = jnp.exp2((scores - top) * (SCALE * LOG2E))
            prob = raw * (1.0 / jnp.sum(raw, axis=0, keepdims=True))
            pb = prob.astype(BF16)
            delta = jnp.sum(pb.astype(F32) * dp, axis=0, keepdims=True)
            ds = prob * (dp - delta)
            zero = jnp.zeros((BLK, BLK), F32)
            pfull = jnp.concatenate(
                [jnp.where(causal, zero, prob[:BLK]).astype(BF16), pb[BLK:], jnp.where(causal, prob[:BLK], zero).astype(BF16)], 0
            )
            dsb = ds.astype(BF16)
            dfull = jnp.concatenate(
                [jnp.where(causal, zero, ds[:BLK]).astype(BF16), dsb[BLK:], jnp.where(causal, ds[:BLK], zero).astype(BF16)], 0
            )
            acc[h, 1, krows, :] += dot(pfull, dob, NN)
            acc[h, 0, krows, :] += dot(dfull, qb, NN)
            dq = dot(kb, dfull, TN)
            qout[h, qrows, :] = (dq.T * SCALE).astype(BF16)

            out_start((2,), h, i)

            @pl.when(jnp.logical_not(first))
            def _():
                retout[h, 0, qrows, :] = (acc[h, 0, qrows, :] * SCALE).astype(BF16)
                retout[h, 1, qrows, :] = acc[h, 1, qrows, :].astype(BF16)
                if at_once:
                    for t in range(2):
                        rt_copy(t, h, i).start()

        if not at_once:

            @pl.when(jnp.logical_not(first))
            def _():
                for off in AWAY:
                    for t in range(2):
                        rt_copy(t, h, lax.rem(col + off, ROW)).start()

    def finish_head(h):
        for off in AWAY:
            j = lax.rem(col + off, ROW)
            rows = block_rows(0, j)
            own = block_rows(OWN, j)
            for t in range(2):
                scale = SCALE if t == 0 else 1.0

                @pl.when(last)
                def _():
                    fin[h, t, rows, :] = (acc[h, t, own, :] * scale).astype(BF16)

                @pl.when(jnp.logical_not(last))
                def _():
                    rt_copy(t, h, j).wait_recv()
                    mine = acc[h, t, own, :] * scale
                    fin[h, t, rows, :] = (mine + retin[h, t, rows, :].astype(F32)).astype(BF16)

            out_start((0, 1), h, j)

    def drain():
        @pl.loop(0, HPD)
        def _(h):
            for t in range(4):
                for off in range(1, ROW):
                    in_copy(t, h, off).wait_send()

            @pl.loop(0, ROW)
            def _(j):
                for t in range(2):

                    @pl.when(jnp.logical_not(last))
                    def _():
                        fw_copy(t, h, j).wait_send()

                    @pl.when(jnp.logical_not(first))
                    def _():
                        rt_copy(t, h, j).wait_send()

                @pl.when(j == col)
                def _():
                    for t in range(3):
                        out_local(t, h).wait()

                @pl.when(j != col)
                def _():
                    for t in range(3):
                        out_remote(t, h, j).wait_send()
                        out_wait(t, h, j)

    def mixer_tables():
        bin32 = bin_ref[0].astype(F32)
        cout32 = cout_ref[0].astype(F32)
        for tab, rows32 in ((btab, bin32), (ctab, cout32)):
            for n in range(NST):
                wide = jnp.broadcast_to(rows32[n : n + 1, :], (TOK, TOK)).T
                for k in range(NCH):
                    natt[pl.ds(k * PITCH, LEN), :] = wide[k * LEN : (k + 1) * LEN]
                for j in range(LEN):
                    tab[n, j] = natt[pl.ds(j, NCH, stride=PITCH), :]

    def spread(block, n):
        return jnp.broadcast_to(block[n : n + 1, :], (NCH, 128))

    def mixer_local(c):
        lanes = pl.ds(pl.multiple_of(c * 128, 128), 128)
        x = x_ref[0, :, lanes].astype(F32)
        z = raw_ref[0, :, lanes].astype(F32) + bias_ref[:, lanes]
        ct = cot_ref[0, :, lanes].astype(F32)
        small = jnp.exp(-jnp.abs(z))
        dt = jnp.maximum(z, 0.0) + jnp.log1p(small)
        sg = jnp.where(z >= 0.0, 1.0, small) / (1.0 + small)
        par[c, 9:10, :] = jnp.sum(ct * x, axis=0, keepdims=True)
        for k in range(NCH):
            rows = pl.ds(k * PITCH, LEN)
            part = slice(k * LEN, (k + 1) * LEN)
            dts[c, rows, :] = dt[part]
            xs[c, rows, :] = x[part]
            cts[c, rows, :] = ct[part]
            sgs[c, rows, :] = sg[part]
        a2 = -jnp.exp(dl_ref[:, lanes]) * LOG2E
        a2s[c] = a2
        rate = [spread(a2, n) for n in range(NST)]
        state = [jnp.zeros((NCH, 128), F32) for _ in range(NST)]
        decay = [jnp.ones((NCH, 128), F32) for _ in range(NST)]
        back = [jnp.zeros((NCH, 128), F32) for _ in range(NST)]
        for j in range(LEN):
            rows = pl.ds(j, NCH, stride=PITCH)
            dtj = dts[c, rows, :]
            uj = dtj * xs[c, rows, :]
            cj = cts[c, rows, :]
            for n in range(NST):
                a = jnp.exp2(dtj * rate[n])
                avs[c, j, n] = a
                state[n] = a * state[n] + uj * btab[n, j]
                decay[n] = a * decay[n]
                back[n] = back[n] + decay[n] * (cj * ctab[n, j])
        for n in range(NST):
            rows = pl.ds(n * NCH, NCH)
            tscr[0, rows, :] = state[n]
            tscr[1, rows, :] = decay[n]
            tscr[2, rows, :] = back[n]
        ek = [tscr[0, pl.ds(k, NST, stride=NCH), :] for k in range(NCH)]
        dk = [tscr[1, pl.ds(k, NST, stride=NCH), :] for k in range(NCH)]
        bk = [tscr[2, pl.ds(k, NST, stride=NCH), :] for k in range(NCH)]
        pd = jnp.ones((NST, 128), F32)
        pe = jnp.zeros((NST, 128), F32)
        for k in range(NCH):
            pds[c, k] = pd
            pes[c, k] = pe
            pe = dk[k] * pe + ek[k]
            pd = dk[k] * pd
        sd = jnp.ones((NST, 128), F32)
        sb = jnp.zeros((NST, 128), F32)
        for k in reversed(range(NCH)):
            sds[c, k] = sd
            sbs[c, k] = sb
            sb = dk[k] * sb + bk[k]
            sd = dk[k] * sd
        tot[c] = jnp.concatenate([pe, sb], 0).astype(BF16)
        dtot[c] = jnp.sum(dt, axis=0, keepdims=True)

    def scatter(src, dst, send, recv):
        @pl.loop(0, TILES)
        def _(j):
            @pl.when(j != s)
            def _():
                pltpu.make_async_remote_copy(
                    src_ref=src.at[j], dst_ref=dst.at[s], send_sem=send, recv_sem=recv,
                    device_id={"seq": j}, device_id_type=MESH,
                ).start()

        @pl.when(s < TILES)
        def _():
            dst[s] = src[s]

    def scatter_wait_recv(dst, sem):
        head = dst.at[pl.ds(0, NSEQ - 1)]
        pltpu.make_async_copy(head, head, sem).wait()

    def tiles_wait(ref, sem):
        @pl.when(s < TILES)
        def _():
            part = ref.at[pl.ds(0, TILES - 1)]
            pltpu.make_async_copy(part, part, sem).wait()

        @pl.when(s >= TILES)
        def _():
            part = ref.at[pl.ds(0, TILES)]
            pltpu.make_async_copy(part, part, sem).wait()

    def spread_out(src_of, dst, send, recv):
        @pl.loop(0, NSEQ)
        def _(i):
            @pl.when(i != s)
            def _():
                pltpu.make_async_remote_copy(
                    src_ref=src_of(i), dst_ref=dst.at[s], send_sem=send, recv_sem=recv,
                    device_id={"seq": i}, device_id_type=MESH,
                ).start()

    def mixer_prefix():
        @pl.when(s < TILES)
        def _():
            scatter_wait_recv(gath, a_recv)
            scatter_wait_recv(gdt, t_recv)
            a2 = a2s[s]
            carry = jnp.zeros((NST, 128), F32)
            for i in range(NSEQ):
                ahead[i] = carry
                carry = jnp.exp2(a2 * gdt[i]) * carry + gath[i].astype(F32)[0:8]
            carry = jnp.zeros((NST, 128), F32)
            for i in reversed(range(NSEQ)):
                cbuf[i] = jnp.concatenate([ahead[i], carry], 0).astype(BF16)
                carry = jnp.exp2(a2 * gdt[i]) * carry + gath[i].astype(F32)[8:16]
            spread_out(lambda i: cbuf.at[i], cin, b_send, b_recv)
            cin[s] = cbuf[s]

    def mixer_back(c):
        lanes = pl.ds(pl.multiple_of(c * 128, 128), 128)
        entering = cin[c].astype(F32)
        hin = entering[0:8]
        gin = entering[8:16]
        for k in range(NCH):
            rows = pl.ds(k * NST, NST)
            tscr[0, rows, :] = pds[c, k] * hin + pes[c, k]
            tscr[1, rows, :] = sds[c, k] * gin + sbs[c, k]
        state = [tscr[0, pl.ds(n, NCH, stride=NST), :] for n in range(NST)]
        a2 = a2s[c]
        for j in range(LEN):
            rows = pl.ds(j, NCH, stride=PITCH)
            uj = dts[c, rows, :] * xs[c, rows, :]
            cj = cts[c, rows, :]
            for n in range(NST):
                ah = avs[c, j, n] * state[n]
                ahs[j, n] = ah
                state[n] = ah + uj * btab[n, j]
                gcacc[n, pl.ds(j * NCH, NCH), :] += cj * state[n]
        adj = [tscr[1, pl.ds(n, NCH, stride=NST), :] for n in range(NST)]
        ga = [jnp.zeros((NCH, 128), F32) for _ in range(NST)]
        rate = [spread(a2, n) for n in range(NST)]
        skip = jnp.broadcast_to(skip_ref[:, lanes], (NCH, 128))
        gb = jnp.zeros((NCH, 128), F32)
        for j in reversed(range(LEN)):
            rows = pl.ds(j, NCH, stride=PITCH)
            dtj = dts[c, rows, :]
            xj = xs[c, rows, :]
            uj = dtj * xj
            cj = cts[c, rows, :]
            proj = None
            gdt = None
            for n in range(NST):
                gn = adj[n] + ctab[n, j] * cj
                gbacc[n, pl.ds(j * NCH, NCH), :] += gn * uj
                w = gn * ahs[j, n]
                ga[n] = ga[n] + w * dtj
                p1 = gn * btab[n, j]
                p2 = w * rate[n]
                proj = p1 if proj is None else proj + p1
                gdt = p2 if gdt is None else gdt + p2
                adj[n] = avs[c, j, n] * gn
            gxt[rows, :] = skip * cj + dtj * proj
            graw = (xj * proj + gdt * LN2) * sgs[c, rows, :]
            grt[rows, :] = graw
            gb = gb + graw
        for n in range(NST):
            tscr[2, pl.ds(n * NCH, NCH), :] = ga[n]
        gsum = tscr[2, pl.ds(0, NST, stride=NCH), :]
        for k in range(1, NCH):
            gsum = gsum + tscr[2, pl.ds(k, NST, stride=NCH), :]
        par[c, 0:8, :] = gsum * (a2 * LN2)
        par[c, 8:9, :] = jnp.sum(gb, axis=0, keepdims=True)
        for k in range(NCH):
            rows = pl.ds(k * PITCH, LEN)
            gx_ref[0, pl.ds(k * LEN, LEN), lanes] = gxt[rows, :].astype(BF16)
            gr_ref[0, pl.ds(k * LEN, LEN), lanes] = grt[rows, :].astype(BF16)

    def mixer_state_grads():
        ones = jnp.ones((8, 128), F32)
        for accum, ref in ((gbacc, gin_ref), (gcacc, gout_ref)):
            for n in range(NST):
                rows = [accum[n, pl.ds(k, LEN, stride=NCH), :] for k in range(NCH)]
                full = jnp.concatenate(rows, 0)
                line = lax.dot_general(
                    ones, full, NT, preferred_element_type=F32, precision=lax.Precision.HIGHEST
                )
                gred[n : n + 1, :] = line[0:1, :]
            ref[0] = gred[...].astype(BF16)

    def params_rows():
        @pl.when(s < TILES)
        def _():
            scatter_wait_recv(pgat, c_recv)
            total = pgat[0]
            for i in range(1, NSEQ):
                total = total + pgat[i]
            psm[...] = total
            p4[g] = total

            @pl.loop(0, NGRP)
            def _(i):
                @pl.when(i != g)
                def _():
                    pltpu.make_async_remote_copy(
                        src_ref=psm, dst_ref=p4.at[g], send_sem=d_send, recv_sem=d_recv,
                        device_id={"grp": i}, device_id_type=MESH,
                    ).start()

    def params_groups():
        @pl.when(s < TILES)
        def _():
            head = p4.at[pl.ds(0, NGRP - 1)]
            pltpu.make_async_copy(head, head, d_recv).wait()
            final = (p4[0] + p4[1]) + (p4[2] + p4[3])
            pfin[...] = final
            pout[s] = final
            spread_out(lambda i: pfin, pout, e_send, e_recv)

    def params_store():
        tiles_wait(pout, e_recv)

        @pl.loop(0, TILES)
        def _(c):
            lanes = pl.ds(pl.multiple_of(c * 128, 128), 128)
            gdec_ref[:, lanes] = pout[c, 0:8, :]
            gbias_ref[:, lanes] = pout[c, 8:9, :]
            gskip_ref[:, lanes] = pout[c, 9:10, :]

    def mixer_drain():
        tiles_wait(tot, a_send)
        tiles_wait(dtot, t_send)
        tiles_wait(par, c_send)

        @pl.when(s < TILES)
        def _():
            part = cbuf.at[pl.ds(0, NSEQ - 1)]
            pltpu.make_async_copy(part, part, b_send).wait()
            part = p4.at[pl.ds(0, NGRP - 1)]
            pltpu.make_async_copy(part, part, d_send).wait()
            part = pgat.at[pl.ds(0, NSEQ - 1)]
            pltpu.make_async_copy(part, part, e_send).wait()

    def run_hooks(hooks, i):
        for at, action in hooks:

            @pl.when(i == at)
            def _():
                action()

    def tiles(body, start, stop, hooks):
        @pl.loop(start, stop)
        def _(c):
            run_hooks(hooks, c)
            body(c)

    K, VV, Q, DO = range(4)

    def send(*pairs):
        def go():
            for t, h in pairs:
                send_in(t, h)

        return go

    send((K, 0), (VV, 0))()
    for h in range(HPD):
        forward_own(h)
    for copy in mix_in[:2]:
        copy.wait()
    mixer_tables()
    for copy in mix_in[2:]:
        copy.wait()
    def pass_on(step):
        hear_rows(step)
        tell_rows(step + 1)

    tiles(
        mixer_local, 0, TILES,
        [(4, send((Q, 0))), (6, lambda: pass_on(0)), (12, lambda: pass_on(1)), (18, lambda: hear_rows(2))],
    )
    scatter(tot, gath, a_send, a_recv)
    scatter(dtot, gdt, t_send, t_recv)
    send((DO, 0))()
    gbacc[...] = jnp.zeros(gbacc.shape, F32)
    gcacc[...] = jnp.zeros(gcacc.shape, F32)
    mixer_prefix()
    forward_rest(0)
    send((K, 1), (VV, 1), (K, 2), (VV, 2), (Q, 1), (DO, 1), (Q, 2), (DO, 2))()
    tiles_wait(cin, b_recv)
    tiles(mixer_back, 0, 13, [(9, lambda: forward_rest(1))])
    attention(0, [(2, lambda: forward_rest(2))])
    tiles(mixer_back, 13, TILES, [])
    scatter(par, pgat, c_send, c_recv)
    mixer_state_grads()
    attention(1, [])
    finish_head(0)
    params_rows()
    attention(2, [], at_once=False)
    finish_head(1)
    params_groups()
    finish_head(2)
    params_store()
    mixer_drain()
    drain()


def store_results(*refs):
    n = len(refs) // 2
    srcs, outs, sems = refs[:n], refs[n : 2 * n], refs[2 * n]
    copies = [pltpu.make_async_copy(a, b, sems.at[i]) for i, (a, b) in enumerate(zip(srcs, outs))]
    for copy in copies:
        copy.start()
    for copy in copies:
        copy.wait()


def per_device(queries, keys, values, cot_attn, x, raw, bin_, cout, cot, decay_log, step_bias, skip_gain):
    vm = pl.BlockSpec(memory_space=pltpu.VMEM)
    hbm = pl.BlockSpec(memory_space=pl.ANY)
    att = jax.ShapeDtypeStruct((1, BLK, 12 * HD), BF16)
    mix = jax.ShapeDtypeStruct((1, TOK, INNER), BF16)
    stt = jax.ShapeDtypeStruct((1, NST, TOK), BF16)
    chan = jax.ShapeDtypeStruct((1, INNER), F32)
    V = pltpu.VMEM
    shapes = (att, att, att, mix, mix, stt, stt, jax.ShapeDtypeStruct((NST, INNER), F32), chan, chan)
    D = pltpu.SemaphoreType.DMA
    scratch = [
        V((HPD, OWN, HD), BF16), V((HPD, OWN, HD), BF16), V((HPD, 2 * OWN, HD), BF16), V((HPD, 2 * OWN, HD), BF16),
        V((HPD, 2, 2 * OWN, HD), F32), V((HPD, OWN, HD), BF16),
        V((HPD, 2, OWN, HD), BF16), V((HPD, 2, OWN, HD), BF16), V((HPD, 2, OWN, HD), BF16),
        *[V((1, TOK, INNER), BF16)] * 3, *[V((1, NST, TOK), BF16)] * 2,
        V((NST, INNER), F32), *[V((1, INNER), F32)] * 2, D((8,)),
        *[V((TILES, NCH * PITCH, 128), F32)] * 4,
        V((TILES, LEN, NST, NCH, 128), F32), V((TILES, NST, 128), F32),
        V((NST, LEN, NCH, 128), F32), V((NST, LEN, NCH, 128), F32), V((NCH * PITCH, 128), F32),
        V((3, NST * NCH, 128), F32),
        *[V((TILES, NCH, NST, 128), F32)] * 4,
        V((TILES, 16, 128), BF16), V((TILES, 1, 128), F32), V((NSEQ, 16, 128), BF16), V((NSEQ, 1, 128), F32),
        V((NSEQ, NST, 128), F32), V((NSEQ, 16, 128), BF16), V((TILES, 16, 128), BF16),
        V((LEN, NST, NCH, 128), F32), V((NCH * PITCH, 128), F32), V((NCH * PITCH, 128), F32),
        V((NST, LEN * NCH, 128), F32), V((NST, LEN * NCH, 128), F32), V((NST, 128), F32),
        V((TILES, 10, 128), F32), V((NSEQ, 10, 128), F32), V((10, 128), F32), V((NGRP, 10, 128), F32),
        V((10, 128), F32), V((TILES, 10, 128), F32),
        pltpu.SemaphoreType.REGULAR((3,)), D((4, HPD, ROW - 1)), D((4, HPD, ROW - 1)), D((4, HPD)),
        *[D((2, HPD, ROW))] * 4,
        D((3, HPD, ROW)), D((3, HPD, ROW)), D((3, HPD)),
        *[D(())] * 12,
    ]
    res = pl.pallas_call(
        kernel,
        out_shape=tuple(V(a.shape, a.dtype) for a in shapes),
        in_specs=[hbm] * 12,
        out_specs=(vm,) * 10,
        scratch_shapes=scratch,
        compiler_params=pltpu.CompilerParams(
            collective_id=0, has_side_effects=True, vmem_limit_bytes=56 * 1024 * 1024
        ),
    )(queries, keys, values, cot_attn, x, raw, bin_, cout, cot, decay_log, step_bias.reshape(1, -1), skip_gain.reshape(1, -1))
    res = pl.pallas_call(
        store_results,
        out_shape=shapes,
        in_specs=[vm] * len(shapes),
        out_specs=(hbm,) * len(shapes),
        scratch_shapes=[D((len(shapes),))],
        compiler_params=pltpu.CompilerParams(vmem_limit_bytes=4 * 1024 * 1024),
    )(*[pltpu.with_memory_space_constraint(a, pltpu.VMEM) for a in res])
    return tuple(res[:8]) + (res[8].reshape(-1), res[9].reshape(-1))


def solution(mesh):
    tok = P("grp", "seq", None)
    stt = P("grp", None, "seq")
    return jax.shard_map(
        per_device,
        mesh=mesh,
        in_specs=(tok,) * 4 + (tok, tok, stt, stt, tok, P(), P(), P()),
        out_specs=(tok,) * 3 + (tok, tok, stt, stt, P(), P(), P()),
        check_vma=False,
    )
```
